128 devices in a mesh: seq: 16 (over y, z), rep: 8 (over x, core).
Axes of the slice: x: 4, y: 4, z: 4, core: 2. Of those that a mesh axis runs over, the one named last changes fastest.
Arguments:
- head_out: bfloat16 [8, 8192, 4096], P('rep', 'seq'), may hold values from -6 to 6
- grad_out: bfloat16 [8, 8192, 3584], P('rep', 'seq'), may hold values from -6 to 6
- hash_codes: int32 [8, 16, 3584], P('rep'), may hold values from 0 to 511
- loss_mask: int32 [8192], P('seq'), may hold values 0 or 1
- query_ids: int32 [64], replicated, may hold values from 0 to 8191
Outputs:
- attribution: float32 [8192, 64], P(('seq', 'rep'))
The draws below stay inside these ranges and needn't reach their ends.
All inputs are finite; a program needn't handle non-finite values. No bound on the sum of `loss_mask` on one device may be relied on, other than what follows from the above.
Results may differ from the reference program's by a relative error of at most 0.0025.
Values may be sent and summed in bfloat16 or wider, within the bound.
No kernel may reach another device: no remote copies, remote signals or barrier semaphores. Data moves between devices by JAX's collectives and lax.ppermute only.
A program may use at most 64 MiB of HBM per device.

```python
import math
import jax
import jax.numpy as jnp
from jax import lax

D = 3584
HEADS = 16
HEAD_DIM = 256
QUERIES = 64
TOKENS = 8192
LAYERS = 8


def set_ends(array, key, low, high):
    place = [jax.random.randint(jax.random.fold_in(key, axis), (), 0, length) for axis, length in enumerate(array.shape)]
    widest = array.shape.index(max(array.shape))
    neighbour = place[:widest] + [(place[widest] + 1) % array.shape[widest]] + place[widest + 1:]
    return array.at[tuple(place)].set(low).at[tuple(neighbour)].set(high)


def shard_levels(own_key, dims, pieces, smallest, high):
    loudness, own = 1.0, jax.random.fold_in(own_key, 6)
    for position, shards_of in pieces:
        heights = jnp.exp(jax.random.uniform(jax.random.fold_in(own, position), (shards_of,), jnp.float32, smallest / len(pieces), high / len(pieces)))
        loudness = loudness * jnp.repeat(heights, dims[position] // shards_of).reshape([-1 if axis == position else 1 for axis in range(len(dims))])
    return loudness


def noise(rng, shape, scale, most, split=(), kind=jnp.bfloat16):
    loudness = shard_levels(rng, shape, split, -0.22, 0.18) if split else 1.0
    drawn = jax.random.normal(rng, shape, jnp.float32) * scale * loudness
    return jnp.minimum(jnp.maximum(drawn, -most), most).astype(kind)


def setup_inputs(seed: int = 0) -> dict:
    key_list = jax.random.split(jax.random.key(seed), 6)
    head_out = noise(key_list[0], (LAYERS, TOKENS, HEADS * HEAD_DIM), 1.0, 6.0, ((0, 8), (1, 16)))
    grad_out = noise(key_list[1], (LAYERS, TOKENS, D), 1.0, 6.0, ((0, 8), (1, 16)))
    hash_codes = set_ends(jax.random.randint(key_list[2], (LAYERS, HEADS, D), 0, 2 * HEAD_DIM), jax.random.fold_in(key_list[2], 1), 0, (2 * HEAD_DIM) - 1).astype(jnp.int32)
    loss_mask = set_ends((jax.random.randint(key_list[3], (TOKENS,), 0, 4) < 3).astype(jnp.int32), jax.random.fold_in(key_list[3], 1), 0, 1)
    query_ids = set_ends(jax.random.randint(key_list[4], (QUERIES,), 0, TOKENS), jax.random.fold_in(key_list[4], 1), 0, TOKENS - 1).astype(jnp.int32)
    return dict(head_out=head_out, grad_out=grad_out, hash_codes=hash_codes, loss_mask=loss_mask, query_ids=query_ids)


ridge_shift = 0.25
norm_floor = 1e-06

def sketch_head(out_cols, grad_t, head_codes):
    sketch_width = out_cols.shape[1]
    bucket = head_codes % sketch_width
    sign_flip = (1 - 2 * (head_codes // sketch_width)).astype(jnp.float32)
    counted = jax.ops.segment_sum(grad_t * sign_flip[:, None], bucket, num_segments=sketch_width)
    sketch_scale = math.sqrt(sketch_width / grad_t.shape[0])
    return (out_cols.astype(jnp.float32) * counted.T * sketch_scale).astype(jnp.bfloat16)

def head_scores(sketch, mask_bf, token_count, query_ids):
    sketch_width = sketch.shape[1]
    gram_sum = jnp.dot((sketch * mask_bf[:, None]).T.astype(jnp.float32), sketch.astype(jnp.float32), preferred_element_type=jnp.float32)
    gram_sum = gram_sum / token_count + ridge_shift * jnp.eye(sketch_width, dtype=jnp.float32)
    chosen = sketch[query_ids].astype(jnp.float32)
    factor = jnp.linalg.cholesky(gram_sum)
    solved = jax.scipy.linalg.cho_solve((factor, True), chosen.T).astype(jnp.bfloat16)
    return jnp.dot(sketch.astype(jnp.float32), solved.astype(jnp.float32), preferred_element_type=jnp.float32)

def reference(head_out, grad_out, hash_codes, loss_mask, query_ids):
    mask_f = loss_mask.astype(jnp.float32)
    mask_bf = loss_mask.astype(jnp.bfloat16)
    token_count = jnp.sum(mask_f) + jnp.float32(1.0)
    score_sum = jnp.zeros((TOKENS, QUERIES), jnp.float32)
    for layer_index in range(LAYERS):
        grad_t = grad_out[layer_index].astype(jnp.float32).T
        outputs = head_out[layer_index]
        codes = hash_codes[layer_index]

        def add_head(carry, head_index):
            out_cols = lax.dynamic_slice_in_dim(outputs, head_index * HEAD_DIM, HEAD_DIM, 1)
            sketch = sketch_head(out_cols, grad_t, codes[head_index])
            return (carry + head_scores(sketch, mask_bf, token_count, query_ids), None)
        score_sum, _ = lax.scan(add_head, score_sum, jnp.arange(HEADS, dtype=jnp.int32))
    norm_sum = lax.optimization_barrier(jnp.sum(mask_f[:, None] * score_sum * score_sum, 0)) / token_count
    return score_sum / jnp.sqrt(norm_sum + norm_floor)
```

```python
import functools
import math

import jax
import jax.numpy as jnp
from jax import lax
from jax.experimental import pallas as pl
from jax.experimental.pallas import tpu as pltpu
from jax.sharding import Mesh
from jax.sharding import PartitionSpec as P

REP = ("rep_0", "rep_1")
SEQ = ("seq_0", "seq_1")
SEQ_REP = ("seq_0", "seq_1", "rep_0", "rep_1")

RIDGE = 0.25
FLOOR = 1e-06
WIDTH = 256
HALF = 128
EXTRA = 16
F32 = jnp.float32
BF16 = jnp.bfloat16


def dot(a, b, ca, cb, precision=None):
    dims = (((ca,), (cb,)), ((), ()))
    return lax.dot_general(a, b, dims, preferred_element_type=F32, precision=precision)


def params(mib=48):
    return pltpu.CompilerParams(vmem_limit_bytes=mib * 2**20)


def sketch_kernel(scale, code_ref, grad_ref, out_ref, mask_ref, local_ref, sketch_ref, pack_ref):
    tokens, width = grad_ref.shape
    queries = local_ref.shape[0]
    codes = code_ref[0]
    bucket = jnp.broadcast_to((codes & (WIDTH - 1)).astype(jnp.int16), (WIDTH, width))
    sign = jnp.broadcast_to((1 - 2 * (codes >> 8)).astype(F32).astype(BF16), (WIDTH, width))
    row = lax.broadcasted_iota(jnp.int32, (WIDTH, width), 0).astype(jnp.int16)
    table = jnp.where(row == bucket, sign, jnp.zeros((), BF16))
    hashed = dot(grad_ref[...], table, 1, 1)
    sketch = (out_ref[...].astype(F32) * hashed * scale).astype(BF16)
    sketch_ref[...] = sketch

    mask = mask_ref[...]
    masked = (sketch.astype(F32) * mask).astype(BF16)
    gram = dot(masked, sketch, 0, 0)
    token = lax.broadcasted_iota(jnp.int32, (queries, tokens), 1)
    picks = jnp.where(token == local_ref[...], 1.0, 0.0).astype(BF16)
    chosen = dot(picks, sketch, 1, 0).astype(BF16)

    upper, lower = gram[:HALF, :HALF], gram[HALF:, HALF:]
    r = lax.broadcasted_iota(jnp.int32, (HALF, HALF), 0)
    c = lax.broadcasted_iota(jnp.int32, (HALF, HALF), 1)
    both = jnp.where(r >= c, upper, lower)
    diagonal = jnp.sum(jnp.where(r == c, lower, 0.0), 0, keepdims=True)
    row16 = lax.broadcasted_iota(jnp.int32, (EXTRA, HALF), 0)
    extra = jnp.where(row16 == 0, diagonal, jnp.where(row16 == 1, jnp.sum(mask), 0.0))

    def put(start, value):
        rows = value.shape[0]
        high = value.astype(BF16)
        pack_ref[0, start : start + rows, :] = high
        start += WIDTH + EXTRA
        pack_ref[0, start : start + rows, :] = (value - high.astype(F32)).astype(BF16)

    put(0, gram[:HALF, HALF:])
    put(HALF, both)
    put(WIDTH, extra)
    start = 2 * (WIDTH + EXTRA)
    pack_ref[0, start : start + queries, :] = chosen[:, :HALF]
    pack_ref[0, start + queries : start + 2 * queries, :] = chosen[:, HALF:]


def build_sketches(head_out, grad_out, codes, mask, local):
    heads, width = codes.shape
    tokens = grad_out.shape[0]
    queries = local.shape[0]
    rows = 2 * (WIDTH + EXTRA) + 2 * queries
    return pl.pallas_call(
        functools.partial(sketch_kernel, math.sqrt(WIDTH / width)),
        grid=(heads,),
        in_specs=[
            pl.BlockSpec((1, 1, width), lambda h: (h, 0, 0)),
            pl.BlockSpec((tokens, width), lambda h: (0, 0)),
            pl.BlockSpec((tokens, WIDTH), lambda h: (0, h)),
            pl.BlockSpec((tokens, 1), lambda h: (0, 0)),
            pl.BlockSpec((queries, 1), lambda h: (0, 0)),
        ],
        out_specs=[
            pl.BlockSpec((tokens, WIDTH), lambda h: (0, h)),
            pl.BlockSpec((1, rows, HALF), lambda h: (h, 0, 0)),
        ],
        out_shape=[
            jax.ShapeDtypeStruct((tokens, heads * WIDTH), BF16),
            jax.ShapeDtypeStruct((heads, rows, HALF), BF16),
        ],
        compiler_params=params(),
        name="sketch",
    )(codes[:, None, :], grad_out, head_out, mask, local)


def solve_kernel(pack_ref, solved_ref, count_ref, work_ref, answer_ref):
    sources = pack_ref.shape[0]
    queries = (pack_ref.shape[1] - 2 * (WIDTH + EXTRA)) // 2

    def add(start, rows):
        total = pack_ref[0, start : start + rows, :].astype(F32)
        for s in range(1, sources):
            total = total + pack_ref[s, start : start + rows, :].astype(F32)
        return total

    low = WIDTH + EXTRA
    side = add(0, HALF) + add(low, HALF)
    both = add(HALF, HALF) + add(low + HALF, HALF)
    extra = add(WIDTH, EXTRA) + add(low + WIDTH, EXTRA)
    left = add(2 * low, queries)
    right = add(2 * low + queries, queries)
    count = extra[1:2, :] + 1.0
    count_ref[...] = jnp.broadcast_to(count, count_ref.shape)

    r = lax.broadcasted_iota(jnp.int32, (HALF, HALF), 0)
    c = lax.broadcasted_iota(jnp.int32, (HALF, HALF), 1)
    flipped = both.T
    upper = jnp.where(r >= c, both, flipped)
    lower = jnp.where(r < c, both, jnp.where(r == c, extra[0:1, :], flipped))
    ridge = jnp.where(r == c, RIDGE, 0.0)
    work_ref[:HALF, :HALF] = upper / count + ridge
    work_ref[:HALF, HALF:] = side / count
    work_ref[HALF:WIDTH, :HALF] = side.T / count
    work_ref[HALF:WIDTH, HALF:] = lower / count + ridge
    work_ref[WIDTH:, :HALF] = left
    work_ref[WIDTH:, HALF:] = right

    gram = work_ref[:WIDTH, :]
    chosen = work_ref[WIDTH:, :]
    rr = lax.broadcasted_iota(jnp.int32, (WIDTH, WIDTH), 0)
    cc = lax.broadcasted_iota(jnp.int32, (WIDTH, WIDTH), 1)
    unit = rr == cc
    trace = jnp.sum(jnp.where(unit, gram, 0.0))
    step = trace / jnp.sum(gram * gram)
    e1 = jnp.where(unit, 1.0, 0.0) - step * gram
    e1b = e1.astype(BF16)
    e2 = dot(e1b, e1b, 1, 0)
    e2b = e2.astype(BF16)
    e4b = dot(e2b, e2b, 1, 0).astype(BF16)

    def rough(rhs):
        y = rhs * step
        for e in (e1b, e2b, e4b):
            y = y + dot(y.astype(BF16), e, 1, 0)
        return y

    y = rough(chosen)
    for _ in range(3):
        y = y + rough(chosen - dot(y, gram, 1, 0, lax.Precision.HIGHEST))
    answer_ref[...] = y
    residual = chosen - dot(y, gram, 1, 0, lax.Precision.HIGHEST)
    fine = jnp.sum(residual * residual) <= 1e-11 * jnp.sum(chosen * chosen)

    @pl.when(jnp.logical_not(fine))
    def _():
        lane = lax.broadcasted_iota(jnp.int32, work_ref.shape, 1)
        lane1 = lax.broadcasted_iota(jnp.int32, (1, WIDTH), 1)

        def pivot(k, carry):
            whole = work_ref[...]
            row = work_ref[pl.ds(k, 1), :]
            value = jnp.sum(jnp.where(lane1 == k, row, 0.0), 1, keepdims=True)
            column = jnp.sum(jnp.where(lane == k, whole, 0.0), 1, keepdims=True)
            factor = jnp.where(lane1 == k, value - 1.0, row) / value
            work_ref[...] = whole - column * factor
            return carry

        lax.fori_loop(0, WIDTH, pivot, 0)
        answer_ref[...] = work_ref[WIDTH:, :]

    solved = answer_ref[...].astype(BF16)
    for s in range(sources):
        solved_ref[s] = solved


def solve(packs):
    sources, rows, _ = packs.shape
    queries = (rows - 2 * (WIDTH + EXTRA)) // 2
    return pl.pallas_call(
        solve_kernel,
        out_shape=[
            jax.ShapeDtypeStruct((sources, queries, WIDTH), BF16),
            jax.ShapeDtypeStruct((8, HALF), F32),
        ],
        scratch_shapes=[
            pltpu.VMEM((WIDTH + queries, WIDTH), F32),
            pltpu.VMEM((queries, WIDTH), F32),
        ],
        compiler_params=params(),
        name="solve",
    )(packs)


def score_kernel(sketch_ref, solved_ref, part_ref):
    heads, queries, _ = solved_ref.shape
    owners = part_ref.shape[0]
    total = None
    for h in range(heads):
        part = dot(sketch_ref[:, h * WIDTH : (h + 1) * WIDTH], solved_ref[h], 1, 1)
        total = part if total is None else total + part
    size = total.shape[0] // owners
    for o in range(owners):
        block = total[o * size : (o + 1) * size]
        part_ref[o] = jnp.concatenate([block[: size // 2], block[size // 2 :]], 1)


def score(sketch, solved, owners):
    queries = solved.shape[1]
    size = sketch.shape[0] // owners
    return pl.pallas_call(
        score_kernel,
        out_shape=jax.ShapeDtypeStruct((owners, size // 2, 2 * queries), F32),
        compiler_params=params(),
        name="score",
    )(sketch, solved)


def square_kernel(part_ref, mask_ref, contrib_ref, square_ref):
    owners = part_ref.shape[0]
    total = part_ref[0]
    for o in range(1, owners):
        total = total + part_ref[o]
    contrib_ref[...] = total
    rows, queries = total.shape[0], total.shape[1] // 2
    mask = mask_ref[...]
    top = jnp.sum(mask[:rows] * total * total, 0, keepdims=True)
    end = jnp.sum(mask[rows:] * total * total, 0, keepdims=True)
    square = top[:, :queries] + end[:, queries:]
    square_ref[...] = jnp.concatenate([square, square], 1)


def squares(parts, mask):
    owners, rows, lanes = parts.shape
    return pl.pallas_call(
        square_kernel,
        out_shape=[
            jax.ShapeDtypeStruct((rows, lanes), F32),
            jax.ShapeDtypeStruct((1, lanes), F32),
        ],
        compiler_params=params(),
        name="squares",
    )(parts, mask)


def finish_kernel(contrib_ref, square_ref, count_ref, result_ref):
    total = jnp.sum(square_ref[...], axis=(0, 1))[None, :]
    root = jnp.sqrt(total / count_ref[0:1, :] + FLOOR)
    scaled = contrib_ref[...] / root
    rows, queries = scaled.shape[0], scaled.shape[1] // 2
    result_ref[:rows, :] = scaled[:, :queries]
    result_ref[rows:, :] = scaled[:, queries:]


def finish(contrib, gathered, count):
    rows, lanes = contrib.shape
    return pl.pallas_call(
        finish_kernel,
        out_shape=jax.ShapeDtypeStruct((2 * rows, lanes // 2), F32),
        compiler_params=params(),
        name="finish",
    )(contrib, gathered, count)


def exchange(array, axis):
    return lax.all_to_all(array, axis, split_axis=0, concat_axis=0, tiled=True)


def from_everyone(array, axis):
    return exchange(jnp.broadcast_to(array, (lax.axis_size(axis), *array.shape)), axis)


def on_device(head_out, grad_out, hash_codes, loss_mask, query_ids):
    tokens = loss_mask.shape[0]
    owners = lax.axis_size(REP)
    size = tokens // owners
    mask = loss_mask.astype(F32)[:, None]
    local = (query_ids - lax.axis_index(SEQ) * tokens)[:, None]
    own_mask = lax.dynamic_slice_in_dim(mask, lax.axis_index(REP) * size, size, 0)
    sketch, packs = build_sketches(head_out[0], grad_out[0], hash_codes[0], mask, local)
    solved, count = solve(exchange(packs, SEQ))
    parts = score(sketch, exchange(solved, SEQ), owners)
    contrib, square = squares(exchange(parts, REP), own_mask)
    square = from_everyone(square, REP).sum(0)
    return finish(contrib, from_everyone(square, SEQ), count)


def solution(mesh):
    torus = Mesh(mesh.devices.reshape(4, 4, 4, 2), SEQ_REP)
    in_specs = (P(REP, SEQ, None), P(REP, SEQ, None), P(REP, None, None), P(SEQ), P())
    out_specs = P(SEQ_REP, None)
    return jax.shard_map(
        on_device, mesh=torus, in_specs=in_specs, out_specs=out_specs, check_vma=False
    )
```

```python
import functools
import math

import jax
import jax.numpy as jnp
from jax import lax
from jax.experimental import pallas as pl
from jax.experimental.pallas import tpu as pltpu
from jax.sharding import Mesh
from jax.sharding import PartitionSpec as P

REP = ("rep_0", "rep_1")
SEQ = ("seq_0", "seq_1")
SEQ_REP = ("seq_0", "seq_1", "rep_0", "rep_1")

RIDGE = 0.25
FLOOR = 1e-06
WIDTH = 256
HALF = 128
EXTRA = 16
TURNS = 12
F32 = jnp.float32
BF16 = jnp.bfloat16


def dot(a, b, ca, cb, precision=None):
    dims = (((ca,), (cb,)), ((), ()))
    return lax.dot_general(a, b, dims, preferred_element_type=F32, precision=precision)


def params(mib=48):
    return pltpu.CompilerParams(vmem_limit_bytes=mib * 2**20)


def sketch_kernel(scale, code_ref, grad_ref, out_ref, mask_ref, query_ref, sketch_ref, pack_ref,
                  hashed_ref, picks_ref):
    tokens, width = grad_ref.shape
    heads = code_ref.shape[0]
    queries = query_ref.shape[1]
    step = pl.program_id(0)

    @pl.when(step == 0)
    def _():
        local = query_ref[...] - lax.axis_index(SEQ) * tokens
        token = lax.broadcasted_iota(jnp.int32, (tokens, queries), 0)
        picks_ref[...] = jnp.where(token == local, 1.0, 0.0).T.astype(BF16)
        hashed_ref[...] = jnp.zeros_like(hashed_ref)

    def hash_head():
        codes = code_ref[pl.ds(step, 1), :]
        bucket = jnp.broadcast_to((codes & (WIDTH - 1)).astype(jnp.int16), (WIDTH, width))
        sign = jnp.broadcast_to((1 - 2 * (codes >> 8)).astype(F32).astype(BF16), (WIDTH, width))
        row = lax.broadcasted_iota(jnp.int32, (WIDTH, width), 0).astype(jnp.int16)
        table = jnp.where(row == bucket, sign, jnp.zeros((), BF16))
        return dot(grad_ref[...], table, 1, 1)

    def finish_head():
        sketch = (out_ref[...].astype(F32) * hashed_ref[...] * scale).astype(BF16)
        sketch_ref[...] = sketch
        mask = mask_ref[...].astype(F32)
        masked = sketch.T * mask.astype(BF16)
        gram = dot(masked, sketch, 1, 0)
        chosen = dot(picks_ref[...], sketch, 1, 0).astype(BF16)

        upper, lower = gram[:HALF, :HALF], gram[HALF:, HALF:]
        r = lax.broadcasted_iota(jnp.int32, (HALF, HALF), 0)
        c = lax.broadcasted_iota(jnp.int32, (HALF, HALF), 1)
        both = jnp.where(r >= c, upper, lower)
        diagonal = jnp.sum(jnp.where(r == c, lower, 0.0), 0, keepdims=True)
        pair = jnp.concatenate([diagonal, jnp.broadcast_to(jnp.sum(mask), (1, HALF))], 0)
        high = pair.astype(BF16).astype(F32)
        extra = jnp.concatenate([high, pair - high, jnp.zeros((EXTRA - 4, HALF), F32)], 0)

        def put(start, value):
            top = value.astype(BF16)
            pack_ref[0, start : start + HALF, :] = top
            start += WIDTH
            pack_ref[0, start : start + HALF, :] = (value - top.astype(F32)).astype(BF16)

        put(0, gram[:HALF, HALF:])
        put(HALF, both)
        start = 2 * WIDTH
        pack_ref[0, start : start + queries, :] = chosen[:, :HALF]
        start += queries
        pack_ref[0, start : start + queries, :] = chosen[:, HALF:]
        start += queries
        pack_ref[0, start:, :] = extra.astype(BF16)

    @pl.when(step < heads)
    def _():
        finish_head()
        hashed_ref[...] = hash_head()

    @pl.when(step == heads)
    def _():
        finish_head()


def build_sketches(head_out, grad_out, codes, mask, query_ids):
    heads, width = codes.shape
    tokens = grad_out.shape[0]
    queries = query_ids.shape[0]
    rows = 2 * WIDTH + 2 * queries + EXTRA
    last = lambda h: jnp.maximum(h - 1, 0)
    return pl.pallas_call(
        functools.partial(sketch_kernel, math.sqrt(WIDTH / width)),
        grid=(heads + 1,),
        in_specs=[
            pl.BlockSpec((heads, width), lambda h: (0, 0)),
            pl.BlockSpec((tokens, width), lambda h: (0, 0)),
            pl.BlockSpec((tokens, WIDTH), lambda h: (0, last(h))),
            pl.BlockSpec((1, tokens), lambda h: (0, 0)),
            pl.BlockSpec((1, queries), lambda h: (0, 0)),
        ],
        out_specs=[
            pl.BlockSpec((tokens, WIDTH), lambda h: (0, last(h))),
            pl.BlockSpec((1, rows, HALF), lambda h: (last(h), 0, 0)),
        ],
        out_shape=[
            jax.ShapeDtypeStruct((tokens, heads * WIDTH), BF16),
            jax.ShapeDtypeStruct((heads, rows, HALF), BF16),
        ],
        scratch_shapes=[
            pltpu.VMEM((tokens, WIDTH), F32),
            pltpu.VMEM((queries, tokens), BF16),
        ],
        compiler_params=params(),
        name="sketch",
    )(codes, grad_out, head_out, mask[None, :], query_ids[None, :])


def solve_kernel(pack_ref, solved_ref, count_ref, work_ref, answer_ref):
    sources = pack_ref.shape[0]
    queries = (pack_ref.shape[1] - 2 * WIDTH - EXTRA) // 2

    def add(start, rows):
        total = pack_ref[0, start : start + rows, :].astype(F32)
        for s in range(1, sources):
            total = total + pack_ref[s, start : start + rows, :].astype(F32)
        return total

    side = add(0, HALF) + add(WIDTH, HALF)
    both = add(HALF, HALF) + add(WIDTH + HALF, HALF)
    left = add(2 * WIDTH, queries)
    right = add(2 * WIDTH + queries, queries)
    extra = add(2 * WIDTH + 2 * queries, EXTRA)
    extra = extra[0:2, :] + extra[2:4, :]
    count = extra[1:2, :] + 1.0
    count_ref[...] = jnp.broadcast_to(count, count_ref.shape)

    r = lax.broadcasted_iota(jnp.int32, (HALF, HALF), 0)
    c = lax.broadcasted_iota(jnp.int32, (HALF, HALF), 1)
    flipped = both.T
    upper = jnp.where(r >= c, both, flipped)
    lower = jnp.where(r < c, both, jnp.where(r == c, extra[0:1, :], flipped))
    ridge = jnp.where(r == c, RIDGE, 0.0)
    work_ref[:HALF, :HALF] = upper / count + ridge
    work_ref[:HALF, HALF:] = side / count
    work_ref[HALF:WIDTH, :HALF] = side.T / count
    work_ref[HALF:WIDTH, HALF:] = lower / count + ridge
    work_ref[WIDTH:, :HALF] = left
    work_ref[WIDTH:, HALF:] = right

    gram = work_ref[:WIDTH, :]
    chosen = work_ref[WIDTH:, :]
    rr = lax.broadcasted_iota(jnp.int32, (WIDTH, WIDTH), 0)
    cc = lax.broadcasted_iota(jnp.int32, (WIDTH, WIDTH), 1)
    unit = rr == cc
    scale = 1.0 / jnp.sum(jnp.where(unit, gram, 0.0), 0, keepdims=True)
    e1b = (jnp.where(unit, 1.0, 0.0) - gram * scale).astype(BF16)
    e2b = dot(e1b, e1b, 1, 0).astype(BF16)
    e4b = dot(e2b, e2b, 1, 0).astype(BF16)
    target = 1e-11 * jnp.sum(chosen * chosen)

    def refine(state):
        turn, answer, rest, _ = state
        y = rest * scale
        for e in (e1b, e2b, e4b):
            y = y + dot(y.astype(BF16), e, 1, 0)
        answer = answer + y
        rest = chosen - dot(answer, gram, 1, 0, lax.Precision.HIGHEST)
        return turn + 1, answer, rest, jnp.sum(rest * rest)

    def unfinished(state):
        turn, _, _, size = state
        return jnp.logical_and(turn < TURNS, jnp.logical_not(size <= target))

    start = (0, jnp.zeros_like(chosen), chosen, jnp.float32(jnp.inf))
    _, answer, _, size = lax.while_loop(unfinished, refine, start)
    answer_ref[...] = answer
    fine = size <= target

    @pl.when(jnp.logical_not(fine))
    def _():
        lane = lax.broadcasted_iota(jnp.int32, work_ref.shape, 1)
        lane1 = lax.broadcasted_iota(jnp.int32, (1, WIDTH), 1)

        def pivot(k, carry):
            whole = work_ref[...]
            row = work_ref[pl.ds(k, 1), :]
            value = jnp.sum(jnp.where(lane1 == k, row, 0.0), 1, keepdims=True)
            column = jnp.sum(jnp.where(lane == k, whole, 0.0), 1, keepdims=True)
            factor = jnp.where(lane1 == k, value - 1.0, row) / value
            work_ref[...] = whole - column * factor
            return carry

        lax.fori_loop(0, WIDTH, pivot, 0)
        answer_ref[...] = work_ref[WIDTH:, :]

    solved = answer_ref[...].astype(BF16)
    for s in range(sources):
        solved_ref[s] = solved


def solve(packs):
    sources, rows, _ = packs.shape
    queries = (rows - 2 * WIDTH - EXTRA) // 2
    return pl.pallas_call(
        solve_kernel,
        out_shape=[
            jax.ShapeDtypeStruct((sources, queries, WIDTH), BF16),
            jax.ShapeDtypeStruct((8, HALF), F32),
        ],
        scratch_shapes=[
            pltpu.VMEM((WIDTH + queries, WIDTH), F32),
            pltpu.VMEM((queries, WIDTH), F32),
        ],
        compiler_params=params(),
        name="solve",
    )(packs)


def score_kernel(sketch_ref, solved_ref, part_ref):
    heads, queries, _ = solved_ref.shape
    owners = part_ref.shape[0]
    total = None
    for h in range(heads):
        part = dot(sketch_ref[:, h * WIDTH : (h + 1) * WIDTH], solved_ref[h], 1, 1)
        total = part if total is None else total + part
    size = total.shape[0] // owners
    for o in range(owners):
        block = total[o * size : (o + 1) * size]
        part_ref[o] = jnp.concatenate([block[: size // 2], block[size // 2 :]], 1)


def score(sketch, solved, owners):
    queries = solved.shape[1]
    size = sketch.shape[0] // owners
    return pl.pallas_call(
        score_kernel,
        out_shape=jax.ShapeDtypeStruct((owners, size // 2, 2 * queries), F32),
        compiler_params=params(),
        name="score",
    )(sketch, solved)


def square_kernel(part_ref, mask_ref, contrib_ref, square_ref):
    owners = part_ref.shape[0]
    total = part_ref[0]
    for o in range(1, owners):
        total = total + part_ref[o]
    contrib_ref[...] = total
    rows, queries = total.shape[0], total.shape[1] // 2
    mask = mask_ref[...]
    top = jnp.sum(mask[:rows] * total * total, 0, keepdims=True)
    end = jnp.sum(mask[rows:] * total * total, 0, keepdims=True)
    square = top[:, :queries] + end[:, queries:]
    square_ref[...] = jnp.concatenate([square, square], 1)


def squares(parts, mask):
    owners, rows, lanes = parts.shape
    return pl.pallas_call(
        square_kernel,
        out_shape=[
            jax.ShapeDtypeStruct((rows, lanes), F32),
            jax.ShapeDtypeStruct((1, lanes), F32),
        ],
        compiler_params=params(),
        name="squares",
    )(parts, mask)


def finish_kernel(contrib_ref, square_ref, count_ref, result_ref):
    total = jnp.sum(square_ref[...], axis=(0, 1))[None, :]
    root = jnp.sqrt(total / count_ref[0:1, :] + FLOOR)
    scaled = contrib_ref[...] / root
    rows, queries = scaled.shape[0], scaled.shape[1] // 2
    result_ref[:rows, :] = scaled[:, :queries]
    result_ref[rows:, :] = scaled[:, queries:]


def finish(contrib, gathered, count):
    rows, lanes = contrib.shape
    return pl.pallas_call(
        finish_kernel,
        out_shape=jax.ShapeDtypeStruct((2 * rows, lanes // 2), F32),
        compiler_params=params(),
        name="finish",
    )(contrib, gathered, count)


def exchange(array, axis):
    return lax.all_to_all(array, axis, split_axis=0, concat_axis=0, tiled=True)


def from_everyone(array, axis):
    return exchange(jnp.broadcast_to(array, (lax.axis_size(axis), *array.shape)), axis)


def on_device(head_out, grad_out, hash_codes, loss_mask, query_ids):
    tokens = loss_mask.shape[0]
    owners = lax.axis_size(REP)
    size = tokens // owners
    own_mask = lax.dynamic_slice_in_dim(loss_mask, lax.axis_index(REP) * size, size, 0)
    own_mask = own_mask.astype(F32)[:, None]
    sketch, packs = build_sketches(head_out[0], grad_out[0], hash_codes[0], loss_mask, query_ids)
    solved, count = solve(exchange(packs, SEQ))
    parts = score(sketch, exchange(solved, SEQ), owners)
    contrib, square = squares(exchange(parts, REP), own_mask)
    square = from_everyone(square, REP).sum(0)
    return finish(contrib, from_everyone(square, SEQ), count)


def solution(mesh):
    torus = Mesh(mesh.devices.reshape(4, 4, 4, 2), SEQ_REP)
    in_specs = (P(REP, SEQ, None), P(REP, SEQ, None), P(REP, None, None), P(SEQ), P())
    out_specs = P(SEQ_REP, None)
    return jax.shard_map(
        on_device, mesh=torus, in_specs=in_specs, out_specs=out_specs, check_vma=False
    )
```

```python
import functools
import math

import jax
import jax.numpy as jnp
from jax import lax
from jax.experimental import pallas as pl
from jax.experimental.pallas import tpu as pltpu
from jax.sharding import Mesh
from jax.sharding import PartitionSpec as P

REP = ("rep_0", "rep_1")
SEQ = ("seq_0", "seq_1")
SEQ_REP = ("seq_0", "seq_1", "rep_0", "rep_1")

RIDGE = 0.25
FLOOR = 1e-06
WIDTH = 256
HALF = 128
EXTRA = 16
TURNS = 12
GROUP = 4
F32 = jnp.float32
BF16 = jnp.bfloat16


def dot(a, b, ca, cb, precision=None):
    dims = (((ca,), (cb,)), ((), ()))
    return lax.dot_general(a, b, dims, preferred_element_type=F32, precision=precision)


def params(mib=48):
    return pltpu.CompilerParams(vmem_limit_bytes=mib * 2**20)


def sketch_kernel(scale, code_ref, grad_ref, out_ref, mask_ref, query_ref, sketch_ref, pack_ref,
                  hashed_ref, picks_ref):
    tokens, width = grad_ref.shape
    queries = query_ref.shape[1]
    group = pack_ref.shape[0]
    steps = code_ref.shape[0] // group
    step = pl.program_id(0)

    def hash_heads():
        tables = []
        for g in range(group):
            codes = code_ref[pl.ds(step * group + g, 1), :]
            bucket = jnp.broadcast_to((codes & (WIDTH - 1)).astype(jnp.int16), (WIDTH, width))
            sign = jnp.broadcast_to((1 - 2 * (codes >> 8)).astype(F32).astype(BF16), (WIDTH, width))
            row = lax.broadcasted_iota(jnp.int32, (WIDTH, width), 0).astype(jnp.int16)
            tables.append(jnp.where(row == bucket, sign, jnp.zeros((), BF16)))
        table = tables[0] if group == 1 else jnp.concatenate(tables, 0)
        hashed_ref[...] = dot(grad_ref[...], table, 1, 1)

    def finish_heads():
        mask = mask_ref[...].astype(F32)
        mask_total = jnp.broadcast_to(jnp.sum(mask), (1, HALF))
        mask = mask.astype(BF16)
        for g in range(group):
            columns = slice(g * WIDTH, (g + 1) * WIDTH)
            sketch = (out_ref[:, columns].astype(F32) * hashed_ref[:, columns] * scale).astype(BF16)
            sketch_ref[:, columns] = sketch
            gram = dot(sketch.T * mask, sketch, 1, 0)
            chosen = dot(picks_ref[...], sketch, 1, 0).astype(BF16)

            upper, lower = gram[:HALF, :HALF], gram[HALF:, HALF:]
            r = lax.broadcasted_iota(jnp.int32, (HALF, HALF), 0)
            c = lax.broadcasted_iota(jnp.int32, (HALF, HALF), 1)
            both = jnp.where(r >= c, upper, lower)
            diagonal = jnp.sum(jnp.where(r == c, lower, 0.0), 0, keepdims=True)
            pair = jnp.concatenate([diagonal, mask_total], 0)
            high = pair.astype(BF16).astype(F32)
            extra = jnp.concatenate([high, pair - high, jnp.zeros((EXTRA - 4, HALF), F32)], 0)
            for start, value in ((0, gram[:HALF, HALF:]), (HALF, both)):
                top = value.astype(BF16)
                pack_ref[g, start : start + HALF, :] = top
                start += WIDTH
                pack_ref[g, start : start + HALF, :] = (value - top.astype(F32)).astype(BF16)
            start = 2 * WIDTH
            pack_ref[g, start : start + queries, :] = chosen[:, :HALF]
            start += queries
            pack_ref[g, start : start + queries, :] = chosen[:, HALF:]
            start += queries
            pack_ref[g, start:, :] = extra.astype(BF16)

    @pl.when(step == 0)
    def _():
        local = query_ref[...] - lax.axis_index(SEQ) * tokens
        token = lax.broadcasted_iota(jnp.int32, (tokens, queries), 0)
        picks_ref[...] = jnp.where(token == local, 1.0, 0.0).T.astype(BF16)
        hash_heads()

    @pl.when(jnp.logical_and(step > 0, step < steps))
    def _():
        finish_heads()
        hash_heads()

    @pl.when(step == steps)
    def _():
        finish_heads()


def build_sketches(head_out, grad_out, codes, mask, query_ids):
    heads, width = codes.shape
    tokens = grad_out.shape[0]
    queries = query_ids.shape[0]
    rows = 2 * WIDTH + 2 * queries + EXTRA
    last = lambda h: jnp.maximum(h - 1, 0)
    small = [codes, mask[None, :], query_ids[None, :]]
    small = [pltpu.with_memory_space_constraint(x, pltpu.HBM) for x in small]
    return pl.pallas_call(
        functools.partial(sketch_kernel, math.sqrt(WIDTH / width)),
        grid=(heads // GROUP + 1,),
        in_specs=[
            pl.BlockSpec((heads, width), lambda h: (0, 0)),
            pl.BlockSpec((tokens, width), lambda h: (0, 0)),
            pl.BlockSpec((tokens, GROUP * WIDTH), lambda h: (0, last(h))),
            pl.BlockSpec((1, tokens), lambda h: (0, 0)),
            pl.BlockSpec((1, queries), lambda h: (0, 0)),
        ],
        out_specs=[
            pl.BlockSpec((tokens, GROUP * WIDTH), lambda h: (0, last(h))),
            pl.BlockSpec((GROUP, rows, HALF), lambda h: (last(h), 0, 0)),
        ],
        out_shape=[
            jax.ShapeDtypeStruct((tokens, heads * WIDTH), BF16),
            pltpu.HBM((heads, rows, HALF), BF16),
        ],
        scratch_shapes=[
            pltpu.VMEM((tokens, GROUP * WIDTH), F32),
            pltpu.VMEM((queries, tokens), BF16),
        ],
        compiler_params=params(),
        name="sketch",
    )(small[0], grad_out, head_out, small[1], small[2])


def solve_kernel(pack_ref, solved_ref, count_ref, work_ref, answer_ref):
    sources = pack_ref.shape[0]
    queries = (pack_ref.shape[1] - 2 * WIDTH - EXTRA) // 2

    def add(start, rows):
        total = pack_ref[0, start : start + rows, :].astype(F32)
        for s in range(1, sources):
            total = total + pack_ref[s, start : start + rows, :].astype(F32)
        return total

    side = add(0, HALF) + add(WIDTH, HALF)
    both = add(HALF, HALF) + add(WIDTH + HALF, HALF)
    left = add(2 * WIDTH, queries)
    right = add(2 * WIDTH + queries, queries)
    extra = add(2 * WIDTH + 2 * queries, EXTRA)
    extra = extra[0:2, :] + extra[2:4, :]
    count = extra[1:2, :] + 1.0
    count_ref[...] = jnp.broadcast_to(count, count_ref.shape)

    r = lax.broadcasted_iota(jnp.int32, (HALF, HALF), 0)
    c = lax.broadcasted_iota(jnp.int32, (HALF, HALF), 1)
    flipped = both.T
    upper = jnp.where(r >= c, both, flipped)
    lower = jnp.where(r < c, both, jnp.where(r == c, extra[0:1, :], flipped))
    ridge = jnp.where(r == c, RIDGE, 0.0)
    work_ref[:HALF, :HALF] = upper / count + ridge
    work_ref[:HALF, HALF:] = side / count
    work_ref[HALF:WIDTH, :HALF] = side.T / count
    work_ref[HALF:WIDTH, HALF:] = lower / count + ridge
    work_ref[WIDTH:, :HALF] = left
    work_ref[WIDTH:, HALF:] = right

    gram = work_ref[:WIDTH, :]
    chosen = work_ref[WIDTH:, :]
    rr = lax.broadcasted_iota(jnp.int32, (WIDTH, WIDTH), 0)
    cc = lax.broadcasted_iota(jnp.int32, (WIDTH, WIDTH), 1)
    unit = rr == cc
    scale = 1.0 / jnp.sum(jnp.where(unit, gram, 0.0), 0, keepdims=True)
    e1b = (jnp.where(unit, 1.0, 0.0) - gram * scale).astype(BF16)
    e2b = dot(e1b, e1b, 1, 0).astype(BF16)
    e4b = dot(e2b, e2b, 1, 0).astype(BF16)
    target = 1e-11 * jnp.sum(chosen * chosen)

    def refine(state):
        turn, answer, rest, _ = state
        y = rest * scale
        for e in (e1b, e2b, e4b):
            y = y + dot(y.astype(BF16), e, 1, 0)
        answer = answer + y
        rest = chosen - dot(answer, gram, 1, 0, lax.Precision.HIGHEST)
        return turn + 1, answer, rest, jnp.sum(rest * rest)

    def unfinished(state):
        turn, _, _, size = state
        return jnp.logical_and(turn < TURNS, jnp.logical_not(size <= target))

    start = (0, jnp.zeros_like(chosen), chosen, jnp.float32(jnp.inf))
    _, answer, _, size = lax.while_loop(unfinished, refine, start)
    answer_ref[...] = answer
    fine = size <= target

    @pl.when(jnp.logical_not(fine))
    def _():
        lane = lax.broadcasted_iota(jnp.int32, work_ref.shape, 1)
        lane1 = lax.broadcasted_iota(jnp.int32, (1, WIDTH), 1)

        def pivot(k, carry):
            whole = work_ref[...]
            row = work_ref[pl.ds(k, 1), :]
            value = jnp.sum(jnp.where(lane1 == k, row, 0.0), 1, keepdims=True)
            column = jnp.sum(jnp.where(lane == k, whole, 0.0), 1, keepdims=True)
            factor = jnp.where(lane1 == k, value - 1.0, row) / value
            work_ref[...] = whole - column * factor
            return carry

        lax.fori_loop(0, WIDTH, pivot, 0)
        answer_ref[...] = work_ref[WIDTH:, :]

    solved = answer_ref[...].astype(BF16)
    for s in range(sources):
        solved_ref[s] = solved


def solve(packs):
    sources, rows, _ = packs.shape
    queries = (rows - 2 * WIDTH - EXTRA) // 2
    return pl.pallas_call(
        solve_kernel,
        out_shape=[
            jax.ShapeDtypeStruct((sources, queries, WIDTH), BF16),
            jax.ShapeDtypeStruct((8, HALF), F32),
        ],
        scratch_shapes=[
            pltpu.VMEM((WIDTH + queries, WIDTH), F32),
            pltpu.VMEM((queries, WIDTH), F32),
        ],
        compiler_params=params(),
        name="solve",
    )(packs)


def score_kernel(sketch_ref, solved_ref, part_ref):
    heads, queries, _ = solved_ref.shape
    owners = part_ref.shape[0]
    total = None
    for h in range(heads):
        part = dot(sketch_ref[:, h * WIDTH : (h + 1) * WIDTH], solved_ref[h], 1, 1)
        total = part if total is None else total + part
    size = total.shape[0] // owners
    for o in range(owners):
        block = total[o * size : (o + 1) * size]
        part_ref[o] = jnp.concatenate([block[: size // 2], block[size // 2 :]], 1)


def score(sketch, solved, owners):
    queries = solved.shape[1]
    size = sketch.shape[0] // owners
    return pl.pallas_call(
        score_kernel,
        out_shape=jax.ShapeDtypeStruct((owners, size // 2, 2 * queries), F32),
        compiler_params=params(),
        name="score",
    )(sketch, solved)


def square_kernel(part_ref, mask_ref, contrib_ref, square_ref):
    owners = part_ref.shape[0]
    total = part_ref[0]
    for o in range(1, owners):
        total = total + part_ref[o]
    contrib_ref[...] = total
    rows, queries = total.shape[0], total.shape[1] // 2
    mask = mask_ref[...]
    top = jnp.sum(mask[:rows] * total * total, 0, keepdims=True)
    end = jnp.sum(mask[rows:] * total * total, 0, keepdims=True)
    square = top[:, :queries] + end[:, queries:]
    square_ref[...] = jnp.concatenate([square, square], 1)


def squares(parts, mask):
    owners, rows, lanes = parts.shape
    return pl.pallas_call(
        square_kernel,
        out_shape=[
            jax.ShapeDtypeStruct((rows, lanes), F32),
            jax.ShapeDtypeStruct((1, lanes), F32),
        ],
        compiler_params=params(),
        name="squares",
    )(parts, mask)


def finish_kernel(contrib_ref, square_ref, count_ref, result_ref):
    total = jnp.sum(square_ref[...], axis=(0, 1))[None, :]
    root = jnp.sqrt(total / count_ref[0:1, :] + FLOOR)
    scaled = contrib_ref[...] / root
    rows, queries = scaled.shape[0], scaled.shape[1] // 2
    result_ref[:rows, :] = scaled[:, :queries]
    result_ref[rows:, :] = scaled[:, queries:]


def finish(contrib, gathered, count):
    rows, lanes = contrib.shape
    return pl.pallas_call(
        finish_kernel,
        out_shape=jax.ShapeDtypeStruct((2 * rows, lanes // 2), F32),
        compiler_params=params(),
        name="finish",
    )(contrib, gathered, count)


def exchange(array, axis):
    return lax.all_to_all(array, axis, split_axis=0, concat_axis=0, tiled=True)


def from_everyone(array, axis):
    return exchange(jnp.broadcast_to(array, (lax.axis_size(axis), *array.shape)), axis)


def on_device(head_out, grad_out, hash_codes, loss_mask, query_ids):
    tokens = loss_mask.shape[0]
    owners = lax.axis_size(REP)
    size = tokens // owners
    own_mask = lax.dynamic_slice_in_dim(loss_mask, lax.axis_index(REP) * size, size, 0)
    own_mask = own_mask.astype(F32)[:, None]
    sketch, packs = build_sketches(head_out[0], grad_out[0], hash_codes[0], loss_mask, query_ids)
    solved, count = solve(exchange(packs, SEQ))
    parts = score(sketch, exchange(solved, SEQ), owners)
    contrib, square = squares(exchange(parts, REP), own_mask)
    square = from_everyone(square, REP).sum(0)
    return finish(contrib, from_everyone(square, SEQ), count)


def solution(mesh):
    torus = Mesh(mesh.devices.reshape(4, 4, 4, 2), SEQ_REP)
    in_specs = (P(REP, SEQ, None), P(REP, SEQ, None), P(REP, None, None), P(SEQ), P())
    out_specs = P(SEQ_REP, None)
    return jax.shard_map(
        on_device, mesh=torus, in_specs=in_specs, out_specs=out_specs, check_vma=False
    )
```

```python
import functools
import math

import jax
import jax.numpy as jnp
from jax import lax
from jax.experimental import pallas as pl
from jax.experimental.pallas import tpu as pltpu
from jax.sharding import Mesh
from jax.sharding import PartitionSpec as P

REP = ("rep_0", "rep_1")
SEQ = ("seq_0", "seq_1")
SEQ_REP = ("seq_0", "seq_1", "rep_0", "rep_1")

RIDGE = 0.25
FLOOR = 1e-06
WIDTH = 256
HALF = 128
EXTRA = 16
TURNS = 12
GROUP = 4
SLOTS = 16
F32 = jnp.float32
BF16 = jnp.bfloat16


def dot(a, b, ca, cb, precision=None):
    dims = (((ca,), (cb,)), ((), ()))
    return lax.dot_general(a, b, dims, preferred_element_type=F32, precision=precision)


def params(mib=48):
    return pltpu.CompilerParams(vmem_limit_bytes=mib * 2**20)


def places(query_ids, tokens):
    shape = (query_ids.shape[1], query_ids.shape[1])
    sub, lane = lax.broadcasted_iota(jnp.int32, shape, 0), lax.broadcasted_iota(jnp.int32, shape, 1)
    across = jnp.broadcast_to(lax.div(query_ids, jnp.int32(tokens)).astype(F32), shape)
    source = jnp.sum(jnp.where(sub == lane, across, 0.0), 1, keepdims=True)
    earlier = jnp.logical_and(across == source, lane < sub)
    return source, jnp.sum(jnp.where(earlier, 1.0, 0.0), 1, keepdims=True)


def sketch_kernel(scale, code_ref, grad_ref, out_ref, mask_ref, query_ref, sketch_ref, pack_ref,
                  chosen_ref, crowded_ref, hashed_ref, picks_ref):
    tokens, width = grad_ref.shape
    queries = query_ref.shape[1]
    group = pack_ref.shape[0]
    steps = code_ref.shape[0] // group
    step = pl.program_id(0)

    def hash_heads():
        tables = []
        for g in range(group):
            codes = code_ref[pl.ds(step * group + g, 1), :]
            bucket = jnp.broadcast_to((codes & (WIDTH - 1)).astype(jnp.int16), (WIDTH, width))
            sign = jnp.broadcast_to((1 - 2 * (codes >> 8)).astype(F32).astype(BF16), (WIDTH, width))
            row = lax.broadcasted_iota(jnp.int32, (WIDTH, width), 0).astype(jnp.int16)
            tables.append(jnp.where(row == bucket, sign, jnp.zeros((), BF16)))
        table = tables[0] if group == 1 else jnp.concatenate(tables, 0)
        hashed_ref[...] = dot(grad_ref[...], table, 1, 1)

    def finish_heads():
        mask = mask_ref[...].astype(F32)
        mask_total = jnp.broadcast_to(jnp.sum(mask), (1, HALF))
        mask = mask.astype(BF16)
        for g in range(group):
            columns = slice(g * WIDTH, (g + 1) * WIDTH)
            sketch = (out_ref[:, columns].astype(F32) * hashed_ref[:, columns] * scale).astype(BF16)
            sketch_ref[:, columns] = sketch
            gram = dot(sketch.T * mask, sketch, 1, 0)
            chosen = dot(picks_ref[...], sketch, 1, 0).astype(BF16)

            upper, lower = gram[:HALF, :HALF], gram[HALF:, HALF:]
            r = lax.broadcasted_iota(jnp.int32, (HALF, HALF), 0)
            c = lax.broadcasted_iota(jnp.int32, (HALF, HALF), 1)
            both = jnp.where(r >= c, upper, lower)
            diagonal = jnp.sum(jnp.where(r == c, lower, 0.0), 0, keepdims=True)
            pair = jnp.concatenate([diagonal, mask_total], 0)
            high = pair.astype(BF16).astype(F32)
            extra = jnp.concatenate([high, pair - high, jnp.zeros((EXTRA - 4, HALF), F32)], 0)
            for start, value in ((0, gram[:HALF, HALF:]), (HALF, both)):
                top = value.astype(BF16)
                pack_ref[g, start : start + HALF, :] = top
                start += WIDTH
                pack_ref[g, start : start + HALF, :] = (value - top.astype(F32)).astype(BF16)
            chosen_ref[g, :queries, :] = chosen[:queries, :HALF]
            chosen_ref[g, queries:, :] = chosen[:queries, HALF:]
            start = 2 * WIDTH
            pack_ref[g, start : start + SLOTS, :] = chosen[queries:, :HALF]
            start += SLOTS
            pack_ref[g, start : start + SLOTS, :] = chosen[queries:, HALF:]
            start += SLOTS
            pack_ref[g, start:, :] = extra.astype(BF16)

    @pl.when(step == 0)
    def _():
        local = query_ref[...] - lax.axis_index(SEQ) * tokens
        token = lax.broadcasted_iota(jnp.int32, (tokens, queries), 0)
        picks = jnp.where(token == local, 1.0, 0.0).T.astype(BF16)
        own = jnp.logical_and(local >= 0, local < tokens)
        before = lax.broadcasted_iota(jnp.int32, (queries, queries), 0)
        before = before < lax.broadcasted_iota(jnp.int32, (queries, queries), 1)
        before = jnp.where(before, 1.0, 0.0).astype(BF16)
        ones = jnp.broadcast_to(jnp.where(own, 1.0, 0.0), (SLOTS, queries))
        rank = dot(ones.astype(BF16), before, 1, 0)
        slot = lax.broadcasted_iota(jnp.int32, (SLOTS, queries), 0).astype(F32)
        slots = jnp.where(rank == slot, ones, 0.0).astype(BF16)
        picks_ref[:queries, :] = picks
        picks_ref[queries:, :] = dot(slots, picks, 1, 0).astype(BF16)
        _, rank = places(query_ref[...], tokens)
        crowded_ref[0, 0] = (jnp.max(rank) >= SLOTS).astype(jnp.int32)
        hash_heads()

    @pl.when(jnp.logical_and(step > 0, step < steps))
    def _():
        finish_heads()
        hash_heads()

    @pl.when(step == steps)
    def _():
        finish_heads()


def build_sketches(head_out, grad_out, codes, mask, query_ids):
    heads, width = codes.shape
    tokens = grad_out.shape[0]
    queries = query_ids.shape[0]
    rows = 2 * WIDTH + 2 * SLOTS + EXTRA
    last = lambda h: jnp.maximum(h - 1, 0)
    held = [codes, mask[None, :], query_ids[None, :], grad_out, head_out]
    held = [pltpu.with_memory_space_constraint(x, pltpu.HBM) for x in held]
    return pl.pallas_call(
        functools.partial(sketch_kernel, math.sqrt(WIDTH / width)),
        grid=(heads // GROUP + 1,),
        in_specs=[
            pl.BlockSpec((heads, width), lambda h: (0, 0)),
            pl.BlockSpec((tokens, width), lambda h: (0, 0)),
            pl.BlockSpec((tokens, GROUP * WIDTH), lambda h: (0, last(h))),
            pl.BlockSpec((1, tokens), lambda h: (0, 0)),
            pl.BlockSpec((1, queries), lambda h: (0, 0)),
        ],
        out_specs=[
            pl.BlockSpec((tokens, GROUP * WIDTH), lambda h: (0, last(h))),
            pl.BlockSpec((GROUP, rows, HALF), lambda h: (last(h), 0, 0)),
            pl.BlockSpec((GROUP, 2 * queries, HALF), lambda h: (last(h), 0, 0)),
            pl.BlockSpec(memory_space=pltpu.SMEM),
        ],
        out_shape=[
            pltpu.HBM((tokens, heads * WIDTH), BF16),
            pltpu.HBM((heads, rows, HALF), BF16),
            pltpu.HBM((heads, 2 * queries, HALF), BF16),
            jax.ShapeDtypeStruct((1, 1), jnp.int32),
        ],
        scratch_shapes=[
            pltpu.VMEM((tokens, GROUP * WIDTH), F32),
            pltpu.VMEM((queries + SLOTS, tokens), BF16),
        ],
        compiler_params=params(),
        name="sketch",
    )(held[0], held[3], held[4], held[1], held[2])


def solve_kernel(tokens, pack_ref, query_ref, spare_ref, solved_ref, count_ref, work_ref, answer_ref):
    sources = pack_ref.shape[0]
    queries = query_ref.shape[1]

    def add(start, rows):
        total = pack_ref[0, start : start + rows, :].astype(F32)
        for s in range(1, sources):
            total = total + pack_ref[s, start : start + rows, :].astype(F32)
        return total

    side = add(0, HALF) + add(WIDTH, HALF)
    both = add(HALF, HALF) + add(WIDTH + HALF, HALF)
    extra = add(2 * WIDTH + 2 * SLOTS, EXTRA)

    source, rank = places(query_ref[...], tokens)
    place = lax.broadcasted_iota(jnp.int32, (queries, sources * SLOTS), 1).astype(F32)
    picks = jnp.where(place == source * SLOTS + rank, 1.0, 0.0).astype(BF16)

    def picked(start):
        rows = [pack_ref[s, start : start + SLOTS, :] for s in range(sources)]
        return dot(picks, jnp.concatenate(rows, 0), 1, 0)

    crowded = jnp.max(rank) >= SLOTS
    left = jnp.where(crowded, spare_ref[:, :HALF], picked(2 * WIDTH))
    right = jnp.where(crowded, spare_ref[:, HALF:], picked(2 * WIDTH + SLOTS))
    extra = extra[0:2, :] + extra[2:4, :]
    count = extra[1:2, :] + 1.0
    count_ref[...] = jnp.broadcast_to(count, count_ref.shape)

    r = lax.broadcasted_iota(jnp.int32, (HALF, HALF), 0)
    c = lax.broadcasted_iota(jnp.int32, (HALF, HALF), 1)
    flipped = both.T
    upper = jnp.where(r >= c, both, flipped)
    lower = jnp.where(r < c, both, jnp.where(r == c, extra[0:1, :], flipped))
    ridge = jnp.where(r == c, RIDGE, 0.0)
    work_ref[:HALF, :HALF] = upper / count + ridge
    work_ref[:HALF, HALF:] = side / count
    work_ref[HALF:WIDTH, :HALF] = side.T / count
    work_ref[HALF:WIDTH, HALF:] = lower / count + ridge
    work_ref[WIDTH:, :HALF] = left
    work_ref[WIDTH:, HALF:] = right

    gram = work_ref[:WIDTH, :]
    chosen = work_ref[WIDTH:, :]
    rr = lax.broadcasted_iota(jnp.int32, (WIDTH, WIDTH), 0)
    cc = lax.broadcasted_iota(jnp.int32, (WIDTH, WIDTH), 1)
    unit = rr == cc
    scale = 1.0 / jnp.sum(jnp.where(unit, gram, 0.0), 0, keepdims=True)
    e1b = (jnp.where(unit, 1.0, 0.0) - gram * scale).astype(BF16)
    e2b = dot(e1b, e1b, 1, 0).astype(BF16)
    e4b = dot(e2b, e2b, 1, 0).astype(BF16)
    target = 1e-11 * jnp.sum(chosen * chosen)

    def refine(state):
        turn, answer, rest, _ = state
        y = rest * scale
        for e in (e1b, e2b, e4b):
            y = y + dot(y.astype(BF16), e, 1, 0)
        answer = answer + y
        rest = chosen - dot(answer, gram, 1, 0, lax.Precision.HIGHEST)
        return turn + 1, answer, rest, jnp.sum(rest * rest)

    def unfinished(state):
        turn, _, _, size = state
        return jnp.logical_and(turn < TURNS, jnp.logical_not(size <= target))

    start = (0, jnp.zeros_like(chosen), chosen, jnp.float32(jnp.inf))
    _, answer, _, size = lax.while_loop(unfinished, refine, start)
    answer_ref[...] = answer
    fine = size <= target

    @pl.when(jnp.logical_not(fine))
    def _():
        lane = lax.broadcasted_iota(jnp.int32, work_ref.shape, 1)
        lane1 = lax.broadcasted_iota(jnp.int32, (1, WIDTH), 1)

        def pivot(k, carry):
            whole = work_ref[...]
            row = work_ref[pl.ds(k, 1), :]
            value = jnp.sum(jnp.where(lane1 == k, row, 0.0), 1, keepdims=True)
            column = jnp.sum(jnp.where(lane == k, whole, 0.0), 1, keepdims=True)
            factor = jnp.where(lane1 == k, value - 1.0, row) / value
            work_ref[...] = whole - column * factor
            return carry

        lax.fori_loop(0, WIDTH, pivot, 0)
        answer_ref[...] = work_ref[WIDTH:, :]

    solved = answer_ref[...].astype(BF16)
    for s in range(sources):
        solved_ref[s] = solved


def solve(packs, query_ids, spare, tokens):
    sources = packs.shape[0]
    queries = query_ids.shape[0]
    return pl.pallas_call(
        functools.partial(solve_kernel, tokens),
        out_shape=[
            jax.ShapeDtypeStruct((sources, queries, WIDTH), BF16),
            jax.ShapeDtypeStruct((8, HALF), F32),
        ],
        scratch_shapes=[
            pltpu.VMEM((WIDTH + queries, WIDTH), F32),
            pltpu.VMEM((queries, WIDTH), F32),
        ],
        compiler_params=params(),
        name="solve",
    )(packs, query_ids[None, :], spare)


def spare_rows(chosen, crowded):
    queries = chosen.shape[1] // 2

    def exchanged(rows):
        total = exchange(rows, SEQ).astype(F32).sum(0)
        return jnp.concatenate([total[:queries], total[queries:]], 1)

    def nothing(rows):
        return jnp.zeros((queries, WIDTH), F32)

    return lax.cond(crowded[0, 0] > 0, exchanged, nothing, chosen)


def score_kernel(sketch_ref, solved_ref, part_ref):
    heads, queries, _ = solved_ref.shape
    owners = part_ref.shape[0]
    solved = jnp.concatenate([solved_ref[h] for h in range(heads)], 1)
    total = dot(sketch_ref[...], solved, 1, 1)
    size = total.shape[0] // owners
    for o in range(owners):
        block = total[o * size : (o + 1) * size]
        part_ref[o] = jnp.concatenate([block[: size // 2], block[size // 2 :]], 1)


def score(sketch, solved, owners):
    queries = solved.shape[1]
    size = sketch.shape[0] // owners
    return pl.pallas_call(
        score_kernel,
        out_shape=jax.ShapeDtypeStruct((owners, size // 2, 2 * queries), F32),
        compiler_params=params(),
        name="score",
    )(sketch, solved)


def square_kernel(part_ref, mask_ref, contrib_ref, square_ref):
    owners = part_ref.shape[0]
    total = part_ref[0]
    for o in range(1, owners):
        total = total + part_ref[o]
    contrib_ref[...] = total
    rows, queries = total.shape[0], total.shape[1] // 2
    mask = mask_ref[...]
    top = jnp.sum(mask[:rows] * total * total, 0, keepdims=True)
    end = jnp.sum(mask[rows:] * total * total, 0, keepdims=True)
    square = top[:, :queries] + end[:, queries:]
    square_ref[...] = jnp.concatenate([square, square], 1)


def squares(parts, mask):
    owners, rows, lanes = parts.shape
    return pl.pallas_call(
        square_kernel,
        out_shape=[
            jax.ShapeDtypeStruct((rows, lanes), F32),
            jax.ShapeDtypeStruct((1, lanes), F32),
        ],
        compiler_params=params(),
        name="squares",
    )(parts, mask)


def finish_kernel(contrib_ref, square_ref, count_ref, result_ref):
    total = jnp.sum(square_ref[...], axis=(0, 1))[None, :]
    root = jnp.sqrt(total / count_ref[0:1, :] + FLOOR)
    scaled = contrib_ref[...] / root
    rows, queries = scaled.shape[0], scaled.shape[1] // 2
    result_ref[:rows, :] = scaled[:, :queries]
    result_ref[rows:, :] = scaled[:, queries:]


def finish(contrib, gathered, count):
    rows, lanes = contrib.shape
    return pl.pallas_call(
        finish_kernel,
        out_shape=jax.ShapeDtypeStruct((2 * rows, lanes // 2), F32),
        compiler_params=params(),
        name="finish",
    )(contrib, gathered, count)


def exchange(array, axis):
    return lax.all_to_all(array, axis, split_axis=0, concat_axis=0, tiled=True)


def from_everyone(array, axis):
    return exchange(jnp.broadcast_to(array, (lax.axis_size(axis), *array.shape)), axis)


def on_device(head_out, grad_out, hash_codes, loss_mask, query_ids):
    tokens = loss_mask.shape[0]
    owners = lax.axis_size(REP)
    size = tokens // owners
    own_mask = lax.dynamic_slice_in_dim(loss_mask, lax.axis_index(REP) * size, size, 0)
    own_mask = own_mask.astype(F32)[:, None]
    sketch, packs, chosen, crowded = build_sketches(
        head_out[0], grad_out[0], hash_codes[0], loss_mask, query_ids
    )
    spare = spare_rows(chosen, crowded)
    solved, count = solve(exchange(packs, SEQ), query_ids, spare, tokens)
    parts = score(sketch, exchange(solved, SEQ), owners)
    contrib, square = squares(exchange(parts, REP), own_mask)
    square = from_everyone(square, REP).sum(0)
    return finish(contrib, from_everyone(square, SEQ), count)


def solution(mesh):
    torus = Mesh(mesh.devices.reshape(4, 4, 4, 2), SEQ_REP)
    in_specs = (P(REP, SEQ, None), P(REP, SEQ, None), P(REP, None, None), P(SEQ), P())
    out_specs = P(SEQ_REP, None)
    return jax.shard_map(
        on_device, mesh=torus, in_specs=in_specs, out_specs=out_specs, check_vma=False
    )
```

```python
import functools
import math

import jax
import jax.numpy as jnp
from jax import lax
from jax.experimental import pallas as pl
from jax.experimental.pallas import tpu as pltpu
from jax.sharding import Mesh
from jax.sharding import PartitionSpec as P

REP = ("rep_0", "rep_1")
SEQ = ("seq_0", "seq_1")
SEQ_REP = ("seq_0", "seq_1", "rep_0", "rep_1")

RIDGE = 0.25
FLOOR = 1e-06
WIDTH = 256
HALF = 128
EXTRA = 8
TURNS = 12
GROUP = 4
SLOTS = 16
F32 = jnp.float32
BF16 = jnp.bfloat16


def dot(a, b, ca, cb, precision=None):
    dims = (((ca,), (cb,)), ((), ()))
    return lax.dot_general(a, b, dims, preferred_element_type=F32, precision=precision)


def params(mib=48):
    return pltpu.CompilerParams(vmem_limit_bytes=mib * 2**20)


def places(query_ids, tokens):
    shape = (query_ids.shape[1], query_ids.shape[1])
    sub, lane = lax.broadcasted_iota(jnp.int32, shape, 0), lax.broadcasted_iota(jnp.int32, shape, 1)
    across = jnp.broadcast_to(lax.div(query_ids, jnp.int32(tokens)).astype(F32), shape)
    source = jnp.sum(jnp.where(sub == lane, across, 0.0), 1, keepdims=True)
    earlier = jnp.logical_and(across == source, lane < sub)
    return source, jnp.sum(jnp.where(earlier, 1.0, 0.0), 1, keepdims=True)


def sketch_kernel(scale, code_ref, grad_ref, out_ref, mask_ref, query_ref, sketch_ref, pack_ref,
                  chosen_ref, crowded_ref, hashed_ref, picks_ref):
    tokens, width = grad_ref.shape
    queries = query_ref.shape[1]
    group = pack_ref.shape[0]
    steps = code_ref.shape[0] // group
    step = pl.program_id(0)

    def hash_heads():
        tables = []
        for g in range(group):
            codes = code_ref[pl.ds(step * group + g, 1), :]
            bucket = jnp.broadcast_to((codes & (WIDTH - 1)).astype(jnp.int16), (WIDTH, width))
            sign = jnp.broadcast_to((1 - 2 * (codes >> 8)).astype(F32).astype(BF16), (WIDTH, width))
            row = lax.broadcasted_iota(jnp.int32, (WIDTH, width), 0).astype(jnp.int16)
            tables.append(jnp.where(row == bucket, sign, jnp.zeros((), BF16)))
        table = tables[0] if group == 1 else jnp.concatenate(tables, 0)
        hashed_ref[...] = dot(grad_ref[...], table, 1, 1)

    def finish_heads():
        mask = mask_ref[...].astype(F32)
        mask_total = jnp.broadcast_to(jnp.sum(mask), (1, HALF))
        mask = mask.astype(BF16)
        for g in range(group):
            columns = slice(g * WIDTH, (g + 1) * WIDTH)
            sketch = (out_ref[:, columns].astype(F32) * hashed_ref[:, columns] * scale).astype(BF16)
            sketch_ref[:, columns] = sketch
            gram = dot(sketch.T * mask, sketch, 1, 0)
            chosen = dot(picks_ref[...], sketch, 1, 0).astype(BF16)

            upper, lower = gram[:HALF, :HALF], gram[HALF:, HALF:]
            r = lax.broadcasted_iota(jnp.int32, (HALF, HALF), 0)
            c = lax.broadcasted_iota(jnp.int32, (HALF, HALF), 1)
            both = jnp.where(r >= c, upper, lower)
            diagonal = jnp.sum(jnp.where(r == c, lower, 0.0), 0, keepdims=True)
            pair = jnp.concatenate([diagonal, mask_total], 0)
            high = pair.astype(BF16).astype(F32)
            extra = jnp.concatenate([high, pair - high, jnp.zeros((EXTRA - 4, HALF), F32)], 0)
            for start, value in ((0, gram[:HALF, HALF:]), (HALF, both)):
                top = value.astype(BF16)
                pack_ref[g, start : start + HALF, :] = top
                start += WIDTH
                pack_ref[g, start : start + HALF, :] = (value - top.astype(F32)).astype(BF16)
            chosen_ref[g, :queries, :] = chosen[:queries, :HALF]
            chosen_ref[g, queries:, :] = chosen[:queries, HALF:]
            start = 2 * WIDTH
            pack_ref[g, start : start + SLOTS, :] = chosen[queries:, :HALF]
            start += SLOTS
            pack_ref[g, start : start + SLOTS, :] = chosen[queries:, HALF:]
            start += SLOTS
            pack_ref[g, start:, :] = extra.astype(BF16)

    @pl.when(step == 0)
    def _():
        local = query_ref[...] - lax.axis_index(SEQ) * tokens
        token = lax.broadcasted_iota(jnp.int32, (tokens, queries), 0)
        picks = jnp.where(token == local, 1.0, 0.0).T.astype(BF16)
        own = jnp.logical_and(local >= 0, local < tokens)
        before = lax.broadcasted_iota(jnp.int32, (queries, queries), 0)
        before = before < lax.broadcasted_iota(jnp.int32, (queries, queries), 1)
        before = jnp.where(before, 1.0, 0.0).astype(BF16)
        ones = jnp.broadcast_to(jnp.where(own, 1.0, 0.0), (SLOTS, queries))
        rank = dot(ones.astype(BF16), before, 1, 0)
        slot = lax.broadcasted_iota(jnp.int32, (SLOTS, queries), 0).astype(F32)
        slots = jnp.where(rank == slot, ones, 0.0).astype(BF16)
        picks_ref[:queries, :] = picks
        picks_ref[queries:, :] = dot(slots, picks, 1, 0).astype(BF16)
        _, rank = places(query_ref[...], tokens)
        crowded_ref[0, 0] = (jnp.max(rank) >= SLOTS).astype(jnp.int32)
        hash_heads()

    @pl.when(jnp.logical_and(step > 0, step < steps))
    def _():
        finish_heads()
        hash_heads()

    @pl.when(step == steps)
    def _():
        finish_heads()


def build_sketches(head_out, grad_out, codes, mask, query_ids):
    heads, width = codes.shape
    tokens = grad_out.shape[0]
    queries = query_ids.shape[0]
    rows = 2 * WIDTH + 2 * SLOTS + EXTRA
    last = lambda h: jnp.maximum(h - 1, 0)
    held = [codes, mask[None, :], query_ids[None, :], grad_out, head_out]
    held = [pltpu.with_memory_space_constraint(x, pltpu.HBM) for x in held]
    return pl.pallas_call(
        functools.partial(sketch_kernel, math.sqrt(WIDTH / width)),
        grid=(heads // GROUP + 1,),
        in_specs=[
            pl.BlockSpec((heads, width), lambda h: (0, 0)),
            pl.BlockSpec((tokens, width), lambda h: (0, 0)),
            pl.BlockSpec((tokens, GROUP * WIDTH), lambda h: (0, last(h))),
            pl.BlockSpec((1, tokens), lambda h: (0, 0)),
            pl.BlockSpec((1, queries), lambda h: (0, 0)),
        ],
        out_specs=[
            pl.BlockSpec((tokens, GROUP * WIDTH), lambda h: (0, last(h))),
            pl.BlockSpec((GROUP, rows, HALF), lambda h: (last(h), 0, 0)),
            pl.BlockSpec((GROUP, 2 * queries, HALF), lambda h: (last(h), 0, 0)),
            pl.BlockSpec(memory_space=pltpu.SMEM),
        ],
        out_shape=[
            pltpu.HBM((tokens, heads * WIDTH), BF16),
            pltpu.HBM((heads, rows, HALF), BF16),
            pltpu.HBM((heads, 2 * queries, HALF), BF16),
            jax.ShapeDtypeStruct((1, 1), jnp.int32),
        ],
        scratch_shapes=[
            pltpu.VMEM((tokens, GROUP * WIDTH), F32),
            pltpu.VMEM((queries + SLOTS, tokens), BF16),
        ],
        compiler_params=params(),
        name="sketch",
    )(held[0], held[3], held[4], held[1], held[2])


def solve_kernel(tokens, pack_ref, query_ref, spare_ref, solved_ref, count_ref, work_ref, answer_ref):
    sources = pack_ref.shape[0]
    queries = query_ref.shape[1]

    def add(start, rows):
        total = pack_ref[0, start : start + rows, :].astype(F32)
        for s in range(1, sources):
            total = total + pack_ref[s, start : start + rows, :].astype(F32)
        return total

    side = add(0, HALF) + add(WIDTH, HALF)
    both = add(HALF, HALF) + add(WIDTH + HALF, HALF)
    extra = add(2 * WIDTH + 2 * SLOTS, EXTRA)

    source, rank = places(query_ref[...], tokens)
    place = lax.broadcasted_iota(jnp.int32, (queries, sources * SLOTS), 1).astype(F32)
    picks = jnp.where(place == source * SLOTS + rank, 1.0, 0.0).astype(BF16)

    def picked(start):
        rows = [pack_ref[s, start : start + SLOTS, :] for s in range(sources)]
        return dot(picks, jnp.concatenate(rows, 0), 1, 0)

    crowded = jnp.max(rank) >= SLOTS
    left = jnp.where(crowded, spare_ref[:, :HALF], picked(2 * WIDTH))
    right = jnp.where(crowded, spare_ref[:, HALF:], picked(2 * WIDTH + SLOTS))
    extra = extra[0:2, :] + extra[2:4, :]
    count = extra[1:2, :] + 1.0
    count_ref[...] = jnp.broadcast_to(count, count_ref.shape)

    r = lax.broadcasted_iota(jnp.int32, (HALF, HALF), 0)
    c = lax.broadcasted_iota(jnp.int32, (HALF, HALF), 1)
    flipped = both.T
    upper = jnp.where(r >= c, both, flipped)
    lower = jnp.where(r < c, both, jnp.where(r == c, extra[0:1, :], flipped))
    ridge = jnp.where(r == c, RIDGE, 0.0)
    work_ref[:HALF, :HALF] = upper / count + ridge
    work_ref[:HALF, HALF:] = side / count
    work_ref[HALF:WIDTH, :HALF] = side.T / count
    work_ref[HALF:WIDTH, HALF:] = lower / count + ridge
    work_ref[WIDTH:, :HALF] = left
    work_ref[WIDTH:, HALF:] = right

    gram = work_ref[:WIDTH, :]
    chosen = work_ref[WIDTH:, :]
    rr = lax.broadcasted_iota(jnp.int32, (WIDTH, WIDTH), 0)
    cc = lax.broadcasted_iota(jnp.int32, (WIDTH, WIDTH), 1)
    unit = rr == cc
    scale = 1.0 / jnp.sum(jnp.where(unit, gram, 0.0), 0, keepdims=True)
    e1b = (jnp.where(unit, 1.0, 0.0) - gram * scale).astype(BF16)
    e2b = dot(e1b, e1b, 1, 0).astype(BF16)
    e4b = dot(e2b, e2b, 1, 0).astype(BF16)
    target = 1e-11 * jnp.sum(chosen * chosen)

    def refine(state):
        turn, answer, rest, _ = state
        y = rest * scale
        for e in (e1b, e2b, e4b):
            y = y + dot(y.astype(BF16), e, 1, 0)
        answer = answer + y
        rest = chosen - dot(answer, gram, 1, 0, lax.Precision.HIGHEST)
        return turn + 1, answer, rest, jnp.sum(rest * rest)

    def unfinished(state):
        turn, _, _, size = state
        return jnp.logical_and(turn < TURNS, jnp.logical_not(size <= target))

    start = (0, jnp.zeros_like(chosen), chosen, jnp.float32(jnp.inf))
    _, answer, _, size = lax.while_loop(unfinished, refine, start)
    answer_ref[...] = answer
    fine = size <= target

    @pl.when(jnp.logical_not(fine))
    def _():
        lane = lax.broadcasted_iota(jnp.int32, work_ref.shape, 1)
        lane1 = lax.broadcasted_iota(jnp.int32, (1, WIDTH), 1)

        def pivot(k, carry):
            whole = work_ref[...]
            row = work_ref[pl.ds(k, 1), :]
            value = jnp.sum(jnp.where(lane1 == k, row, 0.0), 1, keepdims=True)
            column = jnp.sum(jnp.where(lane == k, whole, 0.0), 1, keepdims=True)
            factor = jnp.where(lane1 == k, value - 1.0, row) / value
            work_ref[...] = whole - column * factor
            return carry

        lax.fori_loop(0, WIDTH, pivot, 0)
        answer_ref[...] = work_ref[WIDTH:, :]

    solved = answer_ref[...].astype(BF16)
    for s in range(sources):
        solved_ref[s] = solved


def solve(packs, query_ids, spare, tokens):
    sources = packs.shape[0]
    queries = query_ids.shape[0]
    return pl.pallas_call(
        functools.partial(solve_kernel, tokens),
        out_shape=[
            jax.ShapeDtypeStruct((sources, queries, WIDTH), BF16),
            jax.ShapeDtypeStruct((8, HALF), F32),
        ],
        scratch_shapes=[
            pltpu.VMEM((WIDTH + queries, WIDTH), F32),
            pltpu.VMEM((queries, WIDTH), F32),
        ],
        compiler_params=params(),
        name="solve",
    )(packs, query_ids[None, :], spare)


def spare_rows(chosen, crowded):
    queries = chosen.shape[1] // 2

    def exchanged(rows):
        total = exchange(rows, SEQ).astype(F32).sum(0)
        return jnp.concatenate([total[:queries], total[queries:]], 1)

    def nothing(rows):
        return jnp.zeros((queries, WIDTH), F32)

    return lax.cond(crowded[0, 0] > 0, exchanged, nothing, chosen)


def score_kernel(sketch_ref, solved_ref, part_ref):
    heads, queries, _ = solved_ref.shape
    owners = part_ref.shape[0]
    solved = jnp.concatenate([solved_ref[h] for h in range(heads)], 1)
    total = dot(sketch_ref[...], solved, 1, 1)
    size = total.shape[0] // owners
    for o in range(owners):
        block = total[o * size : (o + 1) * size]
        part_ref[o] = jnp.concatenate([block[: size // 2], block[size // 2 :]], 1)


def score(sketch, solved, owners):
    queries = solved.shape[1]
    size = sketch.shape[0] // owners
    return pl.pallas_call(
        score_kernel,
        out_shape=jax.ShapeDtypeStruct((owners, size // 2, 2 * queries), F32),
        compiler_params=params(),
        name="score",
    )(sketch, solved)


def square_kernel(part_ref, mask_ref, contrib_ref, square_ref):
    owners = part_ref.shape[0]
    total = part_ref[0]
    for o in range(1, owners):
        total = total + part_ref[o]
    contrib_ref[...] = total
    rows, queries = total.shape[0], total.shape[1] // 2
    positions = mask_ref.shape[1]
    shape = (positions // owners, positions)
    first = lax.axis_index(REP) * shape[0]
    own = lax.broadcasted_iota(jnp.int32, shape, 1) == lax.broadcasted_iota(jnp.int32, shape, 0) + first
    mask = jnp.sum(jnp.where(own, mask_ref[...].astype(F32), 0.0), 1, keepdims=True)
    top = jnp.sum(mask[:rows] * total * total, 0, keepdims=True)
    end = jnp.sum(mask[rows:] * total * total, 0, keepdims=True)
    square = top[:, :queries] + end[:, queries:]
    square_ref[...] = jnp.concatenate([square, square], 1)


def squares(parts, mask):
    owners, rows, lanes = parts.shape
    return pl.pallas_call(
        square_kernel,
        out_shape=[
            jax.ShapeDtypeStruct((rows, lanes), F32),
            jax.ShapeDtypeStruct((1, lanes), F32),
        ],
        compiler_params=params(),
        name="squares",
    )(parts, mask[None, :])


def finish_kernel(contrib_ref, square_ref, count_ref, result_ref):
    total = jnp.sum(square_ref[...], axis=(0, 1))[None, :]
    root = jnp.sqrt(total / count_ref[0:1, :] + FLOOR)
    scaled = contrib_ref[...] / root
    rows, queries = scaled.shape[0], scaled.shape[1] // 2
    result_ref[:rows, :] = scaled[:, :queries]
    result_ref[rows:, :] = scaled[:, queries:]


def finish(contrib, gathered, count):
    rows, lanes = contrib.shape
    return pl.pallas_call(
        finish_kernel,
        out_shape=jax.ShapeDtypeStruct((2 * rows, lanes // 2), F32),
        compiler_params=params(),
        name="finish",
    )(contrib, gathered, count)


def exchange(array, axis):
    return lax.all_to_all(array, axis, split_axis=0, concat_axis=0, tiled=True)


def from_everyone(array, axis):
    return exchange(jnp.broadcast_to(array, (lax.axis_size(axis), *array.shape)), axis)


def on_device(head_out, grad_out, hash_codes, loss_mask, query_ids):
    tokens = loss_mask.shape[0]
    owners = lax.axis_size(REP)
    sketch, packs, chosen, crowded = build_sketches(
        head_out[0], grad_out[0], hash_codes[0], loss_mask, query_ids
    )
    spare = spare_rows(chosen, crowded)
    solved, count = solve(exchange(packs, SEQ), query_ids, spare, tokens)
    parts = score(sketch, exchange(solved, SEQ), owners)
    contrib, square = squares(exchange(parts, REP), loss_mask)
    square = from_everyone(square, REP).sum(0)
    return finish(contrib, from_everyone(square, SEQ), count)


def solution(mesh):
    torus = Mesh(mesh.devices.reshape(4, 4, 4, 2), SEQ_REP)
    in_specs = (P(REP, SEQ, None), P(REP, SEQ, None), P(REP, None, None), P(SEQ), P())
    out_specs = P(SEQ_REP, None)
    return jax.shard_map(
        on_device, mesh=torus, in_specs=in_specs, out_specs=out_specs, check_vma=False
    )
```

```python
import functools
import math

import jax
import jax.numpy as jnp
from jax import lax
from jax.experimental import pallas as pl
from jax.experimental.pallas import tpu as pltpu
from jax.sharding import Mesh
from jax.sharding import PartitionSpec as P

REP = ("rep_0", "rep_1")
SEQ = ("seq_0", "seq_1")
SEQ_REP = ("seq_0", "seq_1", "rep_0", "rep_1")

RIDGE = 0.25
FLOOR = 1e-06
WIDTH = 256
HALF = 128
EXTRA = 8
TURNS = 12
GROUP = 4
SLOTS = 16
F32 = jnp.float32
BF16 = jnp.bfloat16


def dot(a, b, ca, cb, precision=None):
    dims = (((ca,), (cb,)), ((), ()))
    return lax.dot_general(a, b, dims, preferred_element_type=F32, precision=precision)


def params(mib=48):
    return pltpu.CompilerParams(vmem_limit_bytes=mib * 2**20)


def places(query_ids, tokens):
    shape = (query_ids.shape[1], query_ids.shape[1])
    sub, lane = lax.broadcasted_iota(jnp.int32, shape, 0), lax.broadcasted_iota(jnp.int32, shape, 1)
    across = jnp.broadcast_to(lax.div(query_ids, jnp.int32(tokens)).astype(F32), shape)
    source = jnp.sum(jnp.where(sub == lane, across, 0.0), 1, keepdims=True)
    earlier = jnp.logical_and(across == source, lane < sub)
    return source, jnp.sum(jnp.where(earlier, 1.0, 0.0), 1, keepdims=True)


def sketch_kernel(scale, code_ref, grad_ref, out_ref, mask_ref, query_ref, sketch_ref, pack_ref,
                  chosen_ref, crowded_ref, hashed_ref, picks_ref):
    tokens, width = grad_ref.shape
    queries = query_ref.shape[1]
    group = pack_ref.shape[0]
    steps = code_ref.shape[0] // group
    step = pl.program_id(0)

    def hash_heads():
        tables = []
        for g in range(group):
            codes = code_ref[pl.ds(step * group + g, 1), :]
            bucket = jnp.broadcast_to((codes & (WIDTH - 1)).astype(jnp.int16), (WIDTH, width))
            sign = jnp.broadcast_to((1 - 2 * (codes >> 8)).astype(F32).astype(BF16), (WIDTH, width))
            row = lax.broadcasted_iota(jnp.int32, (WIDTH, width), 0).astype(jnp.int16)
            tables.append(jnp.where(row == bucket, sign, jnp.zeros((), BF16)))
        table = tables[0] if group == 1 else jnp.concatenate(tables, 0)
        hashed_ref[...] = dot(grad_ref[...], table, 1, 1)

    def finish_heads():
        mask = mask_ref[...].astype(F32)
        mask_total = jnp.broadcast_to(jnp.sum(mask), (1, HALF))
        mask = mask.astype(BF16)
        for g in range(group):
            columns = slice(g * WIDTH, (g + 1) * WIDTH)
            sketch = (out_ref[:, columns].astype(F32) * hashed_ref[:, columns] * scale).astype(BF16)
            sketch_ref[:, columns] = sketch
            sides = jnp.concatenate([sketch.T * mask, picks_ref[...]], 0)
            products = dot(sides, sketch, 1, 0)
            gram, chosen = products[:WIDTH], products[WIDTH:].astype(BF16)

            upper, lower = gram[:HALF, :HALF], gram[HALF:, HALF:]
            r = lax.broadcasted_iota(jnp.int32, (HALF, HALF), 0)
            c = lax.broadcasted_iota(jnp.int32, (HALF, HALF), 1)
            both = jnp.where(r >= c, upper, lower)
            diagonal = jnp.sum(jnp.where(r == c, lower, 0.0), 0, keepdims=True)
            pair = jnp.concatenate([diagonal, mask_total], 0)
            high = pair.astype(BF16).astype(F32)
            extra = jnp.concatenate([high, pair - high, jnp.zeros((EXTRA - 4, HALF), F32)], 0)
            for start, value in ((0, gram[:HALF, HALF:]), (HALF, both)):
                top = value.astype(BF16)
                pack_ref[g, start : start + HALF, :] = top
                start += WIDTH
                pack_ref[g, start : start + HALF, :] = (value - top.astype(F32)).astype(BF16)
            chosen_ref[g, :queries, :] = chosen[:queries, :HALF]
            chosen_ref[g, queries:, :] = chosen[:queries, HALF:]
            start = 2 * WIDTH
            pack_ref[g, start : start + SLOTS, :] = chosen[queries:, :HALF]
            start += SLOTS
            pack_ref[g, start : start + SLOTS, :] = chosen[queries:, HALF:]
            start += SLOTS
            pack_ref[g, start:, :] = extra.astype(BF16)

    @pl.when(step == 0)
    def _():
        local = query_ref[...] - lax.axis_index(SEQ) * tokens
        token = lax.broadcasted_iota(jnp.int32, (tokens, queries), 0)
        picks = jnp.where(token == local, 1.0, 0.0).T.astype(BF16)
        own = jnp.logical_and(local >= 0, local < tokens)
        before = lax.broadcasted_iota(jnp.int32, (queries, queries), 0)
        before = before < lax.broadcasted_iota(jnp.int32, (queries, queries), 1)
        before = jnp.where(before, 1.0, 0.0).astype(BF16)
        ones = jnp.broadcast_to(jnp.where(own, 1.0, 0.0), (SLOTS, queries))
        rank = dot(ones.astype(BF16), before, 1, 0)
        slot = lax.broadcasted_iota(jnp.int32, (SLOTS, queries), 0).astype(F32)
        slots = jnp.where(rank == slot, ones, 0.0).astype(BF16)
        picks_ref[:queries, :] = picks
        picks_ref[queries:, :] = dot(slots, picks, 1, 0).astype(BF16)
        _, rank = places(query_ref[...], tokens)
        crowded_ref[0, 0] = (jnp.max(rank) >= SLOTS).astype(jnp.int32)
        hash_heads()

    @pl.when(jnp.logical_and(step > 0, step < steps))
    def _():
        finish_heads()
        hash_heads()

    @pl.when(step == steps)
    def _():
        finish_heads()


def build_sketches(head_out, grad_out, codes, mask, query_ids):
    heads, width = codes.shape
    tokens = grad_out.shape[0]
    queries = query_ids.shape[0]
    rows = 2 * WIDTH + 2 * SLOTS + EXTRA
    last = lambda h: jnp.maximum(h - 1, 0)
    held = [codes, mask[None, :], query_ids[None, :], grad_out, head_out]
    held = [pltpu.with_memory_space_constraint(x, pltpu.HBM) for x in held]
    return pl.pallas_call(
        functools.partial(sketch_kernel, math.sqrt(WIDTH / width)),
        grid=(heads // GROUP + 1,),
        in_specs=[
            pl.BlockSpec((heads, width), lambda h: (0, 0)),
            pl.BlockSpec((tokens, width), lambda h: (0, 0)),
            pl.BlockSpec((tokens, GROUP * WIDTH), lambda h: (0, last(h))),
            pl.BlockSpec((1, tokens), lambda h: (0, 0)),
            pl.BlockSpec((1, queries), lambda h: (0, 0)),
        ],
        out_specs=[
            pl.BlockSpec((tokens, GROUP * WIDTH), lambda h: (0, last(h))),
            pl.BlockSpec((GROUP, rows, HALF), lambda h: (last(h), 0, 0)),
            pl.BlockSpec((GROUP, 2 * queries, HALF), lambda h: (last(h), 0, 0)),
            pl.BlockSpec(memory_space=pltpu.SMEM),
        ],
        out_shape=[
            pltpu.HBM((tokens, heads * WIDTH), BF16),
            pltpu.HBM((heads, rows, HALF), BF16),
            pltpu.HBM((heads, 2 * queries, HALF), BF16),
            jax.ShapeDtypeStruct((1, 1), jnp.int32),
        ],
        scratch_shapes=[
            pltpu.VMEM((tokens, GROUP * WIDTH), F32),
            pltpu.VMEM((queries + SLOTS, tokens), BF16),
        ],
        compiler_params=params(),
        name="sketch",
    )(held[0], held[3], held[4], held[1], held[2])


def solve_kernel(tokens, pack_ref, query_ref, spare_ref, solved_ref, count_ref, work_ref, answer_ref):
    sources = pack_ref.shape[0]
    queries = query_ref.shape[1]

    def add(start, rows):
        total = pack_ref[0, start : start + rows, :].astype(F32)
        for s in range(1, sources):
            total = total + pack_ref[s, start : start + rows, :].astype(F32)
        return total

    side = add(0, HALF) + add(WIDTH, HALF)
    both = add(HALF, HALF) + add(WIDTH + HALF, HALF)
    extra = add(2 * WIDTH + 2 * SLOTS, EXTRA)

    source, rank = places(query_ref[...], tokens)
    place = lax.broadcasted_iota(jnp.int32, (queries, sources * SLOTS), 1).astype(F32)
    picks = jnp.where(place == source * SLOTS + rank, 1.0, 0.0).astype(BF16)

    def picked(start):
        rows = [pack_ref[s, start : start + SLOTS, :] for s in range(sources)]
        return dot(picks, jnp.concatenate(rows, 0), 1, 0)

    crowded = jnp.max(rank) >= SLOTS
    left = jnp.where(crowded, spare_ref[:, :HALF], picked(2 * WIDTH))
    right = jnp.where(crowded, spare_ref[:, HALF:], picked(2 * WIDTH + SLOTS))
    extra = extra[0:2, :] + extra[2:4, :]
    count = extra[1:2, :] + 1.0
    count_ref[...] = jnp.broadcast_to(count, count_ref.shape)

    r = lax.broadcasted_iota(jnp.int32, (HALF, HALF), 0)
    c = lax.broadcasted_iota(jnp.int32, (HALF, HALF), 1)
    flipped = both.T
    upper = jnp.where(r >= c, both, flipped)
    lower = jnp.where(r < c, both, jnp.where(r == c, extra[0:1, :], flipped))
    ridge = jnp.where(r == c, RIDGE, 0.0)
    work_ref[:HALF, :HALF] = upper / count + ridge
    work_ref[:HALF, HALF:] = side / count
    work_ref[HALF:WIDTH, :HALF] = side.T / count
    work_ref[HALF:WIDTH, HALF:] = lower / count + ridge
    work_ref[WIDTH:, :HALF] = left
    work_ref[WIDTH:, HALF:] = right

    gram = work_ref[:WIDTH, :]
    chosen = work_ref[WIDTH:, :]
    rr = lax.broadcasted_iota(jnp.int32, (WIDTH, WIDTH), 0)
    cc = lax.broadcasted_iota(jnp.int32, (WIDTH, WIDTH), 1)
    unit = rr == cc
    scale = 1.0 / jnp.sum(jnp.where(unit, gram, 0.0), 0, keepdims=True)
    e1b = (jnp.where(unit, 1.0, 0.0) - gram * scale).astype(BF16)
    e2b = dot(e1b, e1b, 1, 0).astype(BF16)
    e4b = dot(e2b, e2b, 1, 0).astype(BF16)
    target = 1e-11 * jnp.sum(chosen * chosen)

    def refine(state):
        turn, answer, rest, _ = state
        y = rest * scale
        for e in (e1b, e2b, e4b):
            y = y + dot(y.astype(BF16), e, 1, 0)
        answer = answer + y
        rest = chosen - dot(answer, gram, 1, 0, lax.Precision.HIGHEST)
        return turn + 1, answer, rest, jnp.sum(rest * rest)

    def unfinished(state):
        turn, _, _, size = state
        return jnp.logical_and(turn < TURNS, jnp.logical_not(size <= target))

    start = (0, jnp.zeros_like(chosen), chosen, jnp.float32(jnp.inf))
    _, answer, _, size = lax.while_loop(unfinished, refine, start)
    answer_ref[...] = answer
    fine = size <= target

    @pl.when(jnp.logical_not(fine))
    def _():
        lane = lax.broadcasted_iota(jnp.int32, work_ref.shape, 1)
        lane1 = lax.broadcasted_iota(jnp.int32, (1, WIDTH), 1)

        def pivot(k, carry):
            whole = work_ref[...]
            row = work_ref[pl.ds(k, 1), :]
            value = jnp.sum(jnp.where(lane1 == k, row, 0.0), 1, keepdims=True)
            column = jnp.sum(jnp.where(lane == k, whole, 0.0), 1, keepdims=True)
            factor = jnp.where(lane1 == k, value - 1.0, row) / value
            work_ref[...] = whole - column * factor
            return carry

        lax.fori_loop(0, WIDTH, pivot, 0)
        answer_ref[...] = work_ref[WIDTH:, :]

    solved = answer_ref[...].astype(BF16)
    for s in range(sources):
        solved_ref[s] = solved


def solve(packs, query_ids, spare, tokens):
    sources = packs.shape[0]
    queries = query_ids.shape[0]
    return pl.pallas_call(
        functools.partial(solve_kernel, tokens),
        out_shape=[
            jax.ShapeDtypeStruct((sources, queries, WIDTH), BF16),
            jax.ShapeDtypeStruct((8, HALF), F32),
        ],
        scratch_shapes=[
            pltpu.VMEM((WIDTH + queries, WIDTH), F32),
            pltpu.VMEM((queries, WIDTH), F32),
        ],
        compiler_params=params(),
        name="solve",
    )(packs, query_ids[None, :], spare)


def spare_rows(chosen, crowded):
    queries = chosen.shape[1] // 2

    def exchanged(rows):
        total = exchange(rows, SEQ).astype(F32).sum(0)
        return jnp.concatenate([total[:queries], total[queries:]], 1)

    def nothing(rows):
        return jnp.zeros((queries, WIDTH), F32)

    return lax.cond(crowded[0, 0] > 0, exchanged, nothing, chosen)


def score_kernel(sketch_ref, solved_ref, part_ref):
    heads, queries, _ = solved_ref.shape
    owners = part_ref.shape[0]
    solved = jnp.concatenate([solved_ref[h] for h in range(heads)], 1)
    total = dot(sketch_ref[...], solved, 1, 1)
    size = total.shape[0] // owners
    for o in range(owners):
        block = total[o * size : (o + 1) * size]
        part_ref[o] = jnp.concatenate([block[: size // 2], block[size // 2 :]], 1)


def score(sketch, solved, owners):
    queries = solved.shape[1]
    size = sketch.shape[0] // owners
    return pl.pallas_call(
        score_kernel,
        out_shape=jax.ShapeDtypeStruct((owners, size // 2, 2 * queries), F32),
        compiler_params=params(),
        name="score",
    )(sketch, solved)


def square_kernel(part_ref, mask_ref, contrib_ref, square_ref):
    owners = part_ref.shape[0]
    total = part_ref[0]
    for o in range(1, owners):
        total = total + part_ref[o]
    contrib_ref[...] = total
    rows, queries = total.shape[0], total.shape[1] // 2
    positions = mask_ref.shape[1]
    shape = (positions // owners, positions)
    first = lax.axis_index(REP) * shape[0]
    own = lax.broadcasted_iota(jnp.int32, shape, 1) == lax.broadcasted_iota(jnp.int32, shape, 0) + first
    mask = jnp.sum(jnp.where(own, mask_ref[...].astype(F32), 0.0), 1, keepdims=True)
    top = jnp.sum(mask[:rows] * total * total, 0, keepdims=True)
    end = jnp.sum(mask[rows:] * total * total, 0, keepdims=True)
    square = top[:, :queries] + end[:, queries:]
    square_ref[...] = jnp.concatenate([square, square], 1)


def squares(parts, mask):
    owners, rows, lanes = parts.shape
    return pl.pallas_call(
        square_kernel,
        out_shape=[
            jax.ShapeDtypeStruct((rows, lanes), F32),
            jax.ShapeDtypeStruct((1, lanes), F32),
        ],
        compiler_params=params(),
        name="squares",
    )(parts, mask[None, :])


def finish_kernel(contrib_ref, square_ref, count_ref, result_ref):
    total = jnp.sum(square_ref[...], axis=(0, 1))[None, :]
    root = jnp.sqrt(total / count_ref[0:1, :] + FLOOR)
    scaled = contrib_ref[...] / root
    rows, queries = scaled.shape[0], scaled.shape[1] // 2
    result_ref[:rows, :] = scaled[:, :queries]
    result_ref[rows:, :] = scaled[:, queries:]


def finish(contrib, gathered, count):
    rows, lanes = contrib.shape
    return pl.pallas_call(
        finish_kernel,
        out_shape=jax.ShapeDtypeStruct((2 * rows, lanes // 2), F32),
        compiler_params=params(),
        name="finish",
    )(contrib, gathered, count)


def exchange(array, axis):
    return lax.all_to_all(array, axis, split_axis=0, concat_axis=0, tiled=True)


def from_everyone(array, axis):
    return exchange(jnp.broadcast_to(array, (lax.axis_size(axis), *array.shape)), axis)


def on_device(head_out, grad_out, hash_codes, loss_mask, query_ids):
    tokens = loss_mask.shape[0]
    owners = lax.axis_size(REP)
    sketch, packs, chosen, crowded = build_sketches(
        head_out[0], grad_out[0], hash_codes[0], loss_mask, query_ids
    )
    spare = spare_rows(chosen, crowded)
    solved, count = solve(exchange(packs, SEQ), query_ids, spare, tokens)
    parts = score(sketch, exchange(solved, SEQ), owners)
    contrib, square = squares(exchange(parts, REP), loss_mask)
    square = from_everyone(square, REP).sum(0)
    return finish(contrib, from_everyone(square, SEQ), count)


def solution(mesh):
    torus = Mesh(mesh.devices.reshape(4, 4, 4, 2), SEQ_REP)
    in_specs = (P(REP, SEQ, None), P(REP, SEQ, None), P(REP, None, None), P(SEQ), P())
    out_specs = P(SEQ_REP, None)
    return jax.shard_map(
        on_device, mesh=torus, in_specs=in_specs, out_specs=out_specs, check_vma=False
    )
```

```python
import functools
import math

import jax
import jax.numpy as jnp
from jax import lax
from jax.experimental import pallas as pl
from jax.experimental.pallas import tpu as pltpu
from jax.sharding import Mesh
from jax.sharding import PartitionSpec as P

REP = ("rep_0", "rep_1")
SEQ = ("seq_0", "seq_1")
SEQ_REP = ("seq_0", "seq_1", "rep_0", "rep_1")

RIDGE = 0.25
FLOOR = 1e-06
WIDTH = 256
HALF = 128
EXTRA = 8
TURNS = 12
GROUP = 4
SLOTS = 16
F32 = jnp.float32
BF16 = jnp.bfloat16


def dot(a, b, ca, cb, precision=None):
    dims = (((ca,), (cb,)), ((), ()))
    return lax.dot_general(a, b, dims, preferred_element_type=F32, precision=precision)


def params(mib=48):
    return pltpu.CompilerParams(vmem_limit_bytes=mib * 2**20)


def places(query_ids, tokens):
    shape = (query_ids.shape[1], query_ids.shape[1])
    sub, lane = lax.broadcasted_iota(jnp.int32, shape, 0), lax.broadcasted_iota(jnp.int32, shape, 1)
    across = jnp.broadcast_to(lax.div(query_ids, jnp.int32(tokens)).astype(F32), shape)
    source = jnp.sum(jnp.where(sub == lane, across, 0.0), 1, keepdims=True)
    earlier = jnp.logical_and(across == source, lane < sub)
    return source, jnp.sum(jnp.where(earlier, 1.0, 0.0), 1, keepdims=True)


def sketch_kernel(scale, code_ref, grad_ref, out_ref, mask_ref, query_ref, sketch_ref, pack_ref,
                  chosen_ref, crowded_ref, hashed_ref, picks_ref):
    tokens, width = grad_ref.shape
    queries = query_ref.shape[1]
    group = pack_ref.shape[0]
    steps = code_ref.shape[0] // group
    step = pl.program_id(0)

    def hash_heads():
        tables = []
        for g in range(group):
            codes = code_ref[pl.ds(step * group + g, 1), :]
            bucket = jnp.broadcast_to((codes & (WIDTH - 1)).astype(jnp.int16), (WIDTH, width))
            sign = jnp.broadcast_to((1 - 2 * (codes >> 8)).astype(F32).astype(BF16), (WIDTH, width))
            row = lax.broadcasted_iota(jnp.int32, (WIDTH, width), 0).astype(jnp.int16)
            tables.append(jnp.where(row == bucket, sign, jnp.zeros((), BF16)))
        table = tables[0] if group == 1 else jnp.concatenate(tables, 0)
        hashed_ref[...] = dot(grad_ref[...], table, 1, 1)

    def finish_heads():
        mask = mask_ref[...].astype(F32)
        mask_total = jnp.broadcast_to(jnp.sum(mask), (1, HALF))
        mask = mask.astype(BF16)
        for g in range(group):
            columns = slice(g * WIDTH, (g + 1) * WIDTH)
            sketch = (out_ref[:, columns].astype(F32) * hashed_ref[:, columns] * scale).astype(BF16)
            sketch_ref[:, columns] = sketch
            sides = jnp.concatenate([sketch.T * mask, picks_ref[...]], 0)
            products = dot(sides, sketch, 1, 0)
            gram, chosen = products[:WIDTH], products[WIDTH:].astype(BF16)

            upper, lower = gram[:HALF, :HALF], gram[HALF:, HALF:]
            r = lax.broadcasted_iota(jnp.int32, (HALF, HALF), 0)
            c = lax.broadcasted_iota(jnp.int32, (HALF, HALF), 1)
            both = jnp.where(r >= c, upper, lower)
            diagonal = jnp.sum(jnp.where(r == c, lower, 0.0), 0, keepdims=True)
            pair = jnp.concatenate([diagonal, mask_total], 0)
            high = pair.astype(BF16).astype(F32)
            extra = jnp.concatenate([high, pair - high, jnp.zeros((EXTRA - 4, HALF), F32)], 0)
            for start, value in ((0, gram[:HALF, HALF:]), (HALF, both)):
                top = value.astype(BF16)
                pack_ref[g, start : start + HALF, :] = top
                start += WIDTH
                pack_ref[g, start : start + HALF, :] = (value - top.astype(F32)).astype(BF16)
            chosen_ref[g, :queries, :] = chosen[:queries, :HALF]
            chosen_ref[g, queries:, :] = chosen[:queries, HALF:]
            start = 2 * WIDTH
            pack_ref[g, start : start + SLOTS, :] = chosen[queries:, :HALF]
            start += SLOTS
            pack_ref[g, start : start + SLOTS, :] = chosen[queries:, HALF:]
            start += SLOTS
            pack_ref[g, start:, :] = extra.astype(BF16)

    @pl.when(step == 0)
    def _():
        local = query_ref[...] - lax.axis_index(SEQ) * tokens
        token = lax.broadcasted_iota(jnp.int32, (tokens, queries), 0)
        picks = jnp.where(token == local, 1.0, 0.0).T.astype(BF16)
        own = jnp.logical_and(local >= 0, local < tokens)
        before = lax.broadcasted_iota(jnp.int32, (queries, queries), 0)
        before = before < lax.broadcasted_iota(jnp.int32, (queries, queries), 1)
        before = jnp.where(before, 1.0, 0.0).astype(BF16)
        ones = jnp.broadcast_to(jnp.where(own, 1.0, 0.0), (SLOTS, queries))
        rank = dot(ones.astype(BF16), before, 1, 0)
        slot = lax.broadcasted_iota(jnp.int32, (SLOTS, queries), 0).astype(F32)
        slots = jnp.where(rank == slot, ones, 0.0).astype(BF16)
        picks_ref[:queries, :] = picks
        picks_ref[queries:, :] = dot(slots, picks, 1, 0).astype(BF16)
        _, rank = places(query_ref[...], tokens)
        crowded_ref[0, 0] = (jnp.max(rank) >= SLOTS).astype(jnp.int32)
        hash_heads()

    @pl.when(jnp.logical_and(step > 0, step < steps))
    def _():
        finish_heads()
        hash_heads()

    @pl.when(step == steps)
    def _():
        finish_heads()


def build_sketches(head_out, grad_out, codes, mask, query_ids):
    heads, width = codes.shape
    tokens = grad_out.shape[0]
    queries = query_ids.shape[0]
    rows = 2 * WIDTH + 2 * SLOTS + EXTRA
    last = lambda h: jnp.maximum(h - 1, 0)
    held = [codes, mask[None, :], query_ids[None, :], grad_out, head_out]
    held = [pltpu.with_memory_space_constraint(x, pltpu.HBM) for x in held]
    return pl.pallas_call(
        functools.partial(sketch_kernel, math.sqrt(WIDTH / width)),
        grid=(heads // GROUP + 1,),
        in_specs=[
            pl.BlockSpec((heads, width), lambda h: (0, 0)),
            pl.BlockSpec((tokens, width), lambda h: (0, 0)),
            pl.BlockSpec((tokens, GROUP * WIDTH), lambda h: (0, last(h))),
            pl.BlockSpec((1, tokens), lambda h: (0, 0)),
            pl.BlockSpec((1, queries), lambda h: (0, 0)),
        ],
        out_specs=[
            pl.BlockSpec((tokens, GROUP * WIDTH), lambda h: (0, last(h))),
            pl.BlockSpec((GROUP, rows, HALF), lambda h: (last(h), 0, 0)),
            pl.BlockSpec((GROUP, 2 * queries, HALF), lambda h: (last(h), 0, 0)),
            pl.BlockSpec(memory_space=pltpu.SMEM),
        ],
        out_shape=[
            pltpu.HBM((tokens, heads * WIDTH), BF16),
            jax.ShapeDtypeStruct((heads, rows, HALF), BF16),
            pltpu.HBM((heads, 2 * queries, HALF), BF16),
            jax.ShapeDtypeStruct((1, 1), jnp.int32),
        ],
        scratch_shapes=[
            pltpu.VMEM((tokens, GROUP * WIDTH), F32),
            pltpu.VMEM((queries + SLOTS, tokens), BF16),
        ],
        compiler_params=params(),
        name="sketch",
    )(held[0], held[3], held[4], held[1], held[2])


def solve_kernel(tokens, pack_ref, query_ref, spare_ref, solved_ref, count_ref, work_ref, answer_ref):
    sources = pack_ref.shape[0]
    queries = query_ref.shape[1]

    def add(start, rows):
        total = pack_ref[0, start : start + rows, :].astype(F32)
        for s in range(1, sources):
            total = total + pack_ref[s, start : start + rows, :].astype(F32)
        return total

    side = add(0, HALF) + add(WIDTH, HALF)
    both = add(HALF, HALF) + add(WIDTH + HALF, HALF)
    extra = add(2 * WIDTH + 2 * SLOTS, EXTRA)

    source, rank = places(query_ref[...], tokens)
    place = lax.broadcasted_iota(jnp.int32, (queries, sources * SLOTS), 1).astype(F32)
    picks = jnp.where(place == source * SLOTS + rank, 1.0, 0.0).astype(BF16)

    def picked(start):
        rows = [pack_ref[s, start : start + SLOTS, :] for s in range(sources)]
        return dot(picks, jnp.concatenate(rows, 0), 1, 0)

    crowded = jnp.max(rank) >= SLOTS
    left = jnp.where(crowded, spare_ref[:, :HALF], picked(2 * WIDTH))
    right = jnp.where(crowded, spare_ref[:, HALF:], picked(2 * WIDTH + SLOTS))
    extra = extra[0:2, :] + extra[2:4, :]
    count = extra[1:2, :] + 1.0
    count_ref[...] = jnp.broadcast_to(count, count_ref.shape)

    r = lax.broadcasted_iota(jnp.int32, (HALF, HALF), 0)
    c = lax.broadcasted_iota(jnp.int32, (HALF, HALF), 1)
    flipped = both.T
    upper = jnp.where(r >= c, both, flipped)
    lower = jnp.where(r < c, both, jnp.where(r == c, extra[0:1, :], flipped))
    ridge = jnp.where(r == c, RIDGE, 0.0)
    work_ref[:HALF, :HALF] = upper / count + ridge
    work_ref[:HALF, HALF:] = side / count
    work_ref[HALF:WIDTH, :HALF] = side.T / count
    work_ref[HALF:WIDTH, HALF:] = lower / count + ridge
    work_ref[WIDTH:, :HALF] = left
    work_ref[WIDTH:, HALF:] = right

    gram = work_ref[:WIDTH, :]
    chosen = work_ref[WIDTH:, :]
    rr = lax.broadcasted_iota(jnp.int32, (WIDTH, WIDTH), 0)
    cc = lax.broadcasted_iota(jnp.int32, (WIDTH, WIDTH), 1)
    unit = rr == cc
    scale = 1.0 / jnp.sum(jnp.where(unit, gram, 0.0), 0, keepdims=True)
    e1b = (jnp.where(unit, 1.0, 0.0) - gram * scale).astype(BF16)
    e2b = dot(e1b, e1b, 1, 0).astype(BF16)
    e4b = dot(e2b, e2b, 1, 0).astype(BF16)
    target = 1e-11 * jnp.sum(chosen * chosen)

    def refine(state):
        turn, answer, rest, _ = state
        y = rest * scale
        for e in (e1b, e2b, e4b):
            y = y + dot(y.astype(BF16), e, 1, 0)
        answer = answer + y
        rest = chosen - dot(answer, gram, 1, 0, lax.Precision.HIGHEST)
        return turn + 1, answer, rest, jnp.sum(rest * rest)

    def unfinished(state):
        turn, _, _, size = state
        return jnp.logical_and(turn < TURNS, jnp.logical_not(size <= target))

    start = (0, jnp.zeros_like(chosen), chosen, jnp.float32(jnp.inf))
    _, answer, _, size = lax.while_loop(unfinished, refine, start)
    answer_ref[...] = answer
    fine = size <= target

    @pl.when(jnp.logical_not(fine))
    def _():
        lane = lax.broadcasted_iota(jnp.int32, work_ref.shape, 1)
        lane1 = lax.broadcasted_iota(jnp.int32, (1, WIDTH), 1)

        def pivot(k, carry):
            whole = work_ref[...]
            row = work_ref[pl.ds(k, 1), :]
            value = jnp.sum(jnp.where(lane1 == k, row, 0.0), 1, keepdims=True)
            column = jnp.sum(jnp.where(lane == k, whole, 0.0), 1, keepdims=True)
            factor = jnp.where(lane1 == k, value - 1.0, row) / value
            work_ref[...] = whole - column * factor
            return carry

        lax.fori_loop(0, WIDTH, pivot, 0)
        answer_ref[...] = work_ref[WIDTH:, :]

    solved = answer_ref[...].astype(BF16)
    for s in range(sources):
        solved_ref[s] = solved


def solve(packs, query_ids, spare, tokens):
    sources = packs.shape[0]
    queries = query_ids.shape[0]
    return pl.pallas_call(
        functools.partial(solve_kernel, tokens),
        out_shape=[
            jax.ShapeDtypeStruct((sources, queries, WIDTH), BF16),
            jax.ShapeDtypeStruct((8, HALF), F32),
        ],
        scratch_shapes=[
            pltpu.VMEM((WIDTH + queries, WIDTH), F32),
            pltpu.VMEM((queries, WIDTH), F32),
        ],
        compiler_params=params(),
        name="solve",
    )(packs, query_ids[None, :], spare)


def spare_rows(chosen, crowded):
    queries = chosen.shape[1] // 2

    def exchanged(rows):
        total = exchange(rows, SEQ).astype(F32).sum(0)
        return jnp.concatenate([total[:queries], total[queries:]], 1)

    def nothing(rows):
        return jnp.zeros((queries, WIDTH), F32)

    return lax.cond(crowded[0, 0] > 0, exchanged, nothing, chosen)


def score_kernel(sketch_ref, solved_ref, part_ref):
    heads, queries, _ = solved_ref.shape
    owners = part_ref.shape[0]
    solved = jnp.concatenate([solved_ref[h] for h in range(heads)], 1)
    total = dot(sketch_ref[...], solved, 1, 1)
    size = total.shape[0] // owners
    for o in range(owners):
        block = total[o * size : (o + 1) * size]
        part_ref[o] = jnp.concatenate([block[: size // 2], block[size // 2 :]], 1)


def score(sketch, solved, owners):
    queries = solved.shape[1]
    size = sketch.shape[0] // owners
    return pl.pallas_call(
        score_kernel,
        out_shape=jax.ShapeDtypeStruct((owners, size // 2, 2 * queries), F32),
        compiler_params=params(),
        name="score",
    )(sketch, solved)


def square_kernel(part_ref, mask_ref, contrib_ref, square_ref):
    owners = part_ref.shape[0]
    total = part_ref[0]
    for o in range(1, owners):
        total = total + part_ref[o]
    contrib_ref[...] = total
    rows, queries = total.shape[0], total.shape[1] // 2
    positions = mask_ref.shape[1]
    shape = (positions // owners, positions)
    first = lax.axis_index(REP) * shape[0]
    own = lax.broadcasted_iota(jnp.int32, shape, 1) == lax.broadcasted_iota(jnp.int32, shape, 0) + first
    mask = jnp.sum(jnp.where(own, mask_ref[...].astype(F32), 0.0), 1, keepdims=True)
    top = jnp.sum(mask[:rows] * total * total, 0, keepdims=True)
    end = jnp.sum(mask[rows:] * total * total, 0, keepdims=True)
    square = top[:, :queries] + end[:, queries:]
    square_ref[...] = jnp.concatenate([square, square], 1)


def squares(parts, mask):
    owners, rows, lanes = parts.shape
    return pl.pallas_call(
        square_kernel,
        out_shape=[
            jax.ShapeDtypeStruct((rows, lanes), F32),
            jax.ShapeDtypeStruct((1, lanes), F32),
        ],
        compiler_params=params(),
        name="squares",
    )(parts, mask[None, :])


def finish_kernel(contrib_ref, square_ref, count_ref, result_ref):
    total = jnp.sum(square_ref[...], axis=(0, 1))[None, :]
    root = jnp.sqrt(total / count_ref[0:1, :] + FLOOR)
    scaled = contrib_ref[...] / root
    rows, queries = scaled.shape[0], scaled.shape[1] // 2
    result_ref[:rows, :] = scaled[:, :queries]
    result_ref[rows:, :] = scaled[:, queries:]


def finish(contrib, gathered, count):
    rows, lanes = contrib.shape
    return pl.pallas_call(
        finish_kernel,
        out_shape=jax.ShapeDtypeStruct((2 * rows, lanes // 2), F32),
        compiler_params=params(),
        name="finish",
    )(contrib, gathered, count)


def exchange(array, axis):
    return lax.all_to_all(array, axis, split_axis=0, concat_axis=0, tiled=True)


def from_everyone(array, axis):
    return exchange(jnp.broadcast_to(array, (lax.axis_size(axis), *array.shape)), axis)


def on_device(head_out, grad_out, hash_codes, loss_mask, query_ids):
    tokens = loss_mask.shape[0]
    owners = lax.axis_size(REP)
    sketch, packs, chosen, crowded = build_sketches(
        head_out[0], grad_out[0], hash_codes[0], loss_mask, query_ids
    )
    spare = spare_rows(chosen, crowded)
    solved, count = solve(exchange(packs, SEQ), query_ids, spare, tokens)
    parts = score(sketch, exchange(solved, SEQ), owners)
    contrib, square = squares(exchange(parts, REP), loss_mask)
    square = from_everyone(square, REP).sum(0)
    return finish(contrib, from_everyone(square, SEQ), count)


def solution(mesh):
    torus = Mesh(mesh.devices.reshape(4, 4, 4, 2), SEQ_REP)
    in_specs = (P(REP, SEQ, None), P(REP, SEQ, None), P(REP, None, None), P(SEQ), P())
    out_specs = P(SEQ_REP, None)
    return jax.shard_map(
        on_device, mesh=torus, in_specs=in_specs, out_specs=out_specs, check_vma=False
    )
```
